32 devices in a mesh: rep: 4 (over x, y), dp: 8 (over z, core).
Axes of the slice: x: 2, y: 2, z: 4, core: 2. Of those that a mesh axis runs over, the one named last changes fastest.
Arguments:
- x: bfloat16 [32, 2048, 1024], P(('rep', 'dp')), parts along dimension 0
- dy: bfloat16 [32, 2048, 1024], P(('rep', 'dp')), parts along dimension 0
- w_gate: bfloat16 [2, 1024, 2816], replicated
- w_up: bfloat16 [2, 1024, 2816], replicated
- w_down: bfloat16 [2, 2816, 1024], replicated
- m_w_gate: float32 [2, 1024, 2816], P(None, 'dp')
- m_w_up: float32 [2, 1024, 2816], P(None, 'dp')
- m_w_down: float32 [2, 2816, 1024], P(None, 'dp')
- v_w_gate: float32 [2, 1024, 2816], P(None, 'dp')
- v_w_up: float32 [2, 1024, 2816], P(None, 'dp')
- v_w_down: float32 [2, 2816, 1024], P(None, 'dp')
Outputs:
- output 1: bfloat16 [8, 1024, 2816], P('rep'), parts along dimension 0
- output 2: bfloat16 [8, 1024, 2816], P('rep'), parts along dimension 0
- output 3: bfloat16 [8, 2816, 1024], P('rep'), parts along dimension 0
- output 4: float32 [8, 1024, 2816], P('rep', 'dp'), parts along dimension 0
- output 5: float32 [8, 1024, 2816], P('rep', 'dp'), parts along dimension 0
- output 6: float32 [8, 2816, 1024], P('rep', 'dp'), parts along dimension 0
- output 7: float32 [8, 1024, 2816], P('rep', 'dp'), parts along dimension 0
- output 8: float32 [8, 1024, 2816], P('rep', 'dp'), parts along dimension 0
- output 9: float32 [8, 2816, 1024], P('rep', 'dp'), parts along dimension 0
There are 4 independent parts. The reference program is written for one: setup_inputs(seed, part) draws one part's arguments, and reference() takes and returns one part's arrays. A program takes and returns all parts, laid end to end along the dimension named above; an argument that names none is the same for every part.
All inputs are finite; a program needn't handle non-finite values.
Results may differ from the reference program's by a relative error of at most 0.02.
Values are sent between devices in bfloat16 or wider.
A program may use at most 2 GiB of HBM per device.

```python
import jax
import jax.numpy as jnp
from jax import lax

SEQUENCES = 8
TOKENS = 2048
D = 1024
FF = 2816
LAYERS = 2
NAMES = ("w_gate", "w_up", "w_down")
SHAPES = {"w_gate": (LAYERS, D, FF), "w_up": (LAYERS, D, FF), "w_down": (LAYERS, FF, D)}


def bump(key, n, height):
    away = (jnp.arange(n, dtype=jnp.int32) - jax.random.randint(key, (), 0, n, jnp.int32)) % n
    return jnp.where(away < n // 8, height, 1.0)


def together(key, own, strength):
    shared = jax.random.normal(key, own.shape[1:], jnp.float32)
    return (own + strength * shared) * lax.rsqrt(1 + strength * strength)


def setup_inputs(seed: int = 0, part: int = 0) -> dict:
    kx, kdy, ka, kb, kz, kf, kh, kl, *keys = jax.random.split(jax.random.key(seed), 8 + 3 * len(NAMES))
    kx, kdy, ka, kb = (jax.random.fold_in(k, part) for k in (kx, kdy, ka, kb))
    kw, km, kv = (keys[i::3] for i in range(3))
    shape = (SEQUENCES, TOKENS, D)
    much_x, much_dy = jax.random.uniform(kz, (2,), jnp.float32, 0.0, 1.0)
    loud = 2.0 ** jax.random.uniform(jax.random.fold_in(kz, 1), (), jnp.float32, -1.0, 2.0)
    layers = 2.0 ** jax.random.uniform(kl, (LAYERS, 1, 1), jnp.float32, -1.0, 1.0)
    x = together(ka, jax.random.normal(kx, shape, jnp.float32), much_x) * bump(kf, D, 4.0)
    dy = together(kb, jax.random.normal(kdy, shape, jnp.float32), much_dy)
    drawn = {"x": x.astype(jnp.bfloat16), "dy": (loud * dy * (SEQUENCES * TOKENS) ** -0.5).astype(jnp.bfloat16)}
    for key, name in zip(kw, NAMES, strict=True):
        w = jax.random.normal(key, SHAPES[name], jnp.float32) * SHAPES[name][1] ** -0.5
        drawn[name] = (w * {"w_gate": 1.0, "w_up": bump(kh, FF, 4.0), "w_down": layers}[name]).astype(jnp.bfloat16)
    for key, name in zip(km, NAMES, strict=True):
        drawn[f"m_{name}"] = 0.1 * jax.random.normal(key, SHAPES[name], jnp.float32)
    for key, name in zip(kv, NAMES, strict=True):
        drawn[f"v_{name}"] = jax.random.uniform(key, SHAPES[name], jnp.float32, 0.005, 0.015)
    return drawn


def matmul(a, w):
    return jnp.dot(a, w, preferred_element_type=jnp.float32).astype(jnp.bfloat16)


def normed(h):
    wide = h.astype(jnp.float32)
    scale = lax.rsqrt(jnp.mean(wide**2, -1, keepdims=True) + 1e-6)
    return (wide * scale).astype(jnp.bfloat16)


def layer(h, w):
    a = normed(h)
    gate = jnp.dot(a, w["w_gate"], preferred_element_type=jnp.float32)
    up = jnp.dot(a, w["w_up"], preferred_element_type=jnp.float32)
    return h + matmul((jax.nn.silu(gate) * up).astype(jnp.bfloat16), w["w_down"])


def adamw(w, m, v, g):
    m = 0.9 * m + 0.1 * g
    v = 0.95 * v + 0.05 * g * g
    step = m * lax.rsqrt(v + 1e-8) + 0.1 * w
    return (w - 0.02 * step).astype(jnp.bfloat16), m, v


def stack(weights, h):
    return lax.scan(lambda h, w: (layer(h, w), None), h, weights)[0]


def reference(x, dy, w_gate, w_up, w_down, m_w_gate, m_w_up, m_w_down, v_w_gate, v_w_up, v_w_down):
    weights = dict(zip(NAMES, (w_gate, w_up, w_down), strict=True))

    def take(so_far, sequence):
        h, by_y = sequence
        _, back = jax.vjp(lambda w: stack(w, h), weights)
        return jax.tree.map(lambda total, term: total + term.astype(jnp.float32), so_far, back(by_y)[0]), None

    none_yet = {name: jnp.zeros(w.shape, jnp.float32) for name, w in weights.items()}
    by_weights, _ = lax.scan(take, none_yet, (x, dy))
    gradients = [by_weights[name].astype(jnp.bfloat16).astype(jnp.float32) for name in NAMES]
    new = [
        adamw(w.astype(jnp.float32), m, v, g)
        for w, m, v, g in zip((w_gate, w_up, w_down), (m_w_gate, m_w_up, m_w_down), (v_w_gate, v_w_up, v_w_down), gradients, strict=True)
    ]
    return tuple(one[which] for which in range(3) for one in new)
```

```python
import functools

import jax
import jax.numpy as jnp
from jax import lax
from jax.experimental import pallas as pl
from jax.experimental.pallas import tpu as pltpu
from jax.sharding import PartitionSpec as P

MESH = pl.DeviceIdType.MESH
BF, F32 = jnp.bfloat16, jnp.float32
CHIPS = 4
HOP = 2
SLOTS = 12
KEPT = 4
FAR = 1 + HOP * (CHIPS - 1)


def dot(a, b, dims):
    return lax.dot_general(a, b, (dims, ((), ())), preferred_element_type=F32)


def adamw(w, m, v, g):
    m = 0.9 * m + 0.1 * g
    v = 0.95 * v + 0.05 * g * g
    step = m * lax.rsqrt(v + 1e-8) + 0.1 * w
    return (w - 0.02 * step).astype(BF), m, v


def gates(gate, up, d_hidden):
    s = jax.nn.sigmoid(gate)
    gs = gate * s
    return (gs * up).astype(BF), (d_hidden * up * (s + gs * (1 - s))).astype(BF), (d_hidden * gs).astype(BF)


def kernel(dims, *refs):
    D, FF, T, C = dims
    (a2_ref, h1_ref, dy_ref, a1_ref, hid1_ref, gate1_ref, up1_ref, wg_ref, wu_ref, wd_ref) = refs[:10]
    m_refs, v_refs = refs[10:13], refs[13:16]
    wp_ref, mp_ref, vp_ref, hid2_ref, dg2_ref, du2_ref = refs[16:22]
    (A, B, E, acc, hid, dg, du, wgc, wuc, wdc, own, ex, R, L, mi, vi, wi, mo, vo, wo) = refs[22:42]
    (ex_s, ex_r, R_s, R_r, L_s, L_r, AR_s, AR_r, AL_s, AL_r, AD_s, AD_r) = refs[42:54]
    (big_sem, w_sem, row_sem, out_sem, in_sem, put_sem) = refs[54:]

    NC = FF // C
    Q = 6 * NC
    RB, RD, ND = D // 8, C // 8, D // C
    EVEN2, DOWN2, EVEN1, DOWN1 = 0, 2 * NC, 3 * NC, 5 * NC
    TT = min(T, 1024)

    me = lax.axis_index("dp")
    c, k = me // 2, me % 2
    partner, right, left = me + 1 - 2 * k, me + 2, me - 2

    barrier = pltpu.get_barrier_semaphore()
    for there, ok in ((partner, None), (right, c < CHIPS - 1), (left, c > 0)):
        def greet(there=there):
            pl.semaphore_signal(barrier, inc=1, device_id={"dp": there}, device_id_type=MESH)
        greet() if ok is None else pl.when(ok)(greet)

    def load(src, dst, sem):
        return pltpu.make_async_copy(src, dst, sem)

    def send(src, dst, s, r, there):
        return pltpu.make_async_remote_copy(src, dst, s, r, device_id={"dp": there}, device_id_type=MESH)

    def valid(q):
        return (q >= 0) & (q < Q)

    def ex_copy(q):
        s = q % SLOTS
        return send(own.at[s, 1 - k], ex.at[s], ex_s.at[s], ex_r.at[s], partner)

    def R_copy(q, b):
        s = q % SLOTS
        return send(R.at[s, b], R.at[s, b], R_s.at[s, b], R_r.at[s, b], right)

    def L_copy(q, b):
        s = q % SLOTS
        return send(L.at[s, b], L.at[s, b], L_s.at[s, b], L_r.at[s, b], left)

    def all_gather_copy(q, b, there, s_sem, r_sem):
        s, at = q % SLOTS, wp_ref.at[q, 2 * b + k]
        return send(at, at, s_sem.at[s, b], r_sem.at[s, b], there)

    def AR_copy(q, b):
        return all_gather_copy(q, b, right, AR_s, AR_r)

    def AL_copy(q, b):
        return all_gather_copy(q, b, left, AL_s, AL_r)

    def AD_copy(q, b):
        return all_gather_copy(q, b, partner, AD_s, AD_r)

    def pieces(q, whole, wide, do):
        layer = jnp.where(q < EVEN1, 1, 0)
        at = jnp.where(q < EVEN1, q, q - EVEN1)
        for which in (0, 1):
            @pl.when((at < DOWN2) & (at % 2 == which))
            def _():
                whole(which, layer, pl.multiple_of(at // 2 * C, C))
        @pl.when(at >= DOWN2)
        def _():
            wide(2, layer, pl.multiple_of((at - DOWN2) * RD, RD))

    def fetch(q, act):
        s = q % KEPT

        def whole(which, layer, column):
            cols = pl.ds(column, C)
            act(load(m_refs[which].at[layer, :, cols], mi.at[s], in_sem.at[s, 0, 0]))
            act(load(v_refs[which].at[layer, :, cols], vi.at[s], in_sem.at[s, 1, 0]))
            w = (wg_ref, wu_ref)[which]
            act(load(w.at[layer, pl.ds(pl.multiple_of(me * RB, RB), RB), cols], wi.at[s], in_sem.at[s, 2, 0]))

        def wide(which, layer, row):
            for p in range(ND):
                cols, to = pl.ds(p * C, C), pl.ds(p * RD, RD)
                act(load(m_refs[2].at[layer, pl.ds(row, RD), cols], mi.at[s, to], in_sem.at[s, 0, p]))
                act(load(v_refs[2].at[layer, pl.ds(row, RD), cols], vi.at[s, to], in_sem.at[s, 1, p]))
                rows = pl.ds(pl.multiple_of(me * (FF // 8) + row, RD), RD)
                act(load(wd_ref.at[layer, rows, cols], wi.at[s, to], in_sem.at[s, 2, p]))

        pieces(q, whole, wide, None)

    def puts(q):
        s = q % KEPT
        return (
            load(mo.at[s], mp_ref.at[q], put_sem.at[s, 0]),
            load(vo.at[s], vp_ref.at[q], put_sem.at[s, 1]),
            load(wo.at[s], wp_ref.at[q, me], put_sem.at[s, 2]),
        )

    def own_sends(q, act):
        s, n = q % KEPT, q % SLOTS
        to = wp_ref.at[q, me]

        @pl.when(c < CHIPS - 1)
        def _():
            act(send(wo.at[s], to, AR_s.at[n, c], AR_r.at[n, c], right))

        @pl.when(c > 0)
        def _():
            act(send(wo.at[s], to, AL_s.at[n, c], AL_r.at[n, c], left))

        act(send(wo.at[s], to, AD_s.at[n, c], AD_r.at[n, c], partner))

    def start(copy):
        copy.start()

    def wait(copy):
        copy.wait()

    def wait_send(copy):
        copy.wait_send()

    def service(t):
        @pl.when(valid(t - 1))
        def _():
            ex_copy(t - 1).wait_recv()

        q = t - 1 - HOP * c

        @pl.when(valid(q))
        def _():
            s = q % SLOTS
            for b in range(1, CHIPS):
                @pl.when((c > 0) & (b >= c))
                def _():
                    R_copy(q, b).wait_recv()
            for b in range(1, CHIPS):
                @pl.when((c > 0) & (b > c))
                def _():
                    R[s, b] = (own[s, k, b].astype(F32) + ex[s, b].astype(F32) + R[s, b].astype(F32)).astype(BF)

                @pl.when(c == 0)
                def _():
                    R[s, b] = (own[s, k, b].astype(F32) + ex[s, b].astype(F32)).astype(BF)

        p = t - 1 - HOP * (CHIPS - 1 - c)

        @pl.when(valid(p))
        def _():
            s = p % SLOTS
            for b in range(CHIPS - 1):
                @pl.when((c < CHIPS - 1) & (b <= c))
                def _():
                    L_copy(p, b).wait_recv()
            for b in range(CHIPS - 1):
                @pl.when((c < CHIPS - 1) & (b < c))
                def _():
                    L[s, b] = (own[s, k, b].astype(F32) + ex[s, b].astype(F32) + L[s, b].astype(F32)).astype(BF)

                @pl.when(c == CHIPS - 1)
                def _():
                    L[s, b] = (own[s, k, b].astype(F32) + ex[s, b].astype(F32)).astype(BF)

        @pl.when(valid(q))
        def _():
            for b in range(1, CHIPS):
                @pl.when(b > c)
                def _():
                    R_copy(q, b).start()

        @pl.when(valid(p))
        def _():
            for b in range(CHIPS - 1):
                @pl.when(b < c)
                def _():
                    L_copy(p, b).start()

        for b in range(CHIPS):
            q_r = t - FAR - HOP * (c - b)

            @pl.when((b < c) & valid(q_r))
            def _():
                AR_copy(q_r, b).wait_recv()
                @pl.when(c < CHIPS - 1)
                def _():
                    AR_copy(q_r, b).start()
                AD_copy(q_r, b).start()

            q_l = t - FAR - HOP * (b - c)

            @pl.when((b > c) & valid(q_l))
            def _():
                AL_copy(q_l, b).wait_recv()
                @pl.when(c > 0)
                def _():
                    AL_copy(q_l, b).start()
                AD_copy(q_l, b).start()

            far = jnp.abs(c - b)
            q_d = t - 1 - FAR - HOP * far

            @pl.when(valid(q_d))
            def _():
                AD_copy(q_d, b).wait_recv()

            q_s = t - 2 - FAR - HOP * far

            @pl.when(valid(q_s) & (b != c))
            def _():
                @pl.when((b < c) & (c < CHIPS - 1))
                def _():
                    AR_copy(q_s, b).wait_send()
                @pl.when((b > c) & (c > 0))
                def _():
                    AL_copy(q_s, b).wait_send()
                AD_copy(q_s, b).wait_send()

        q_e = t - FAR - 1

        @pl.when(valid(q_e))
        def _():
            ex_copy(q_e).wait_send()
            for b in range(CHIPS):
                if b > 0:
                    @pl.when(b > c)
                    def _():
                        R_copy(q_e, b).wait_send()
                if b < CHIPS - 1:
                    @pl.when(b < c)
                    def _():
                        L_copy(q_e, b).wait_send()

        q_o = t - FAR - 2

        @pl.when(valid(q_o))
        def _():
            for copy in puts(q_o):
                copy.wait()
            own_sends(q_o, wait_send)

        q_m = t - FAR + 2

        @pl.when(valid(q_m))
        def _():
            fetch(q_m, start)

        q_f = t - FAR

        @pl.when(valid(q_f))
        def _():
            fetch(q_f, wait)
            s, o = q_f % SLOTS, q_f % KEPT
            g = own[s, k, c].astype(F32) + ex[s, c].astype(F32) + R[s, c].astype(F32) + L[s, c].astype(F32)
            g = g.astype(BF).astype(F32)
            w, m, v = adamw(wi[o].astype(F32), mi[o], vi[o], g)
            wo[o], mo[o], vo[o] = w, m, v
            for copy in puts(q_f):
                copy.start()
            own_sends(q_f, start)

    def gate_loads(layer, j, act):
        s, at = j % 2, pl.ds(pl.multiple_of(j * C, C), C)
        act(load(wg_ref.at[layer, :, at], wgc.at[s], w_sem.at[s, 0]))
        act(load(wu_ref.at[layer, :, at], wuc.at[s], w_sem.at[s, 1]))

    def down_load(layer, j, act):
        s, at = j % 2, pl.ds(pl.multiple_of(j * C, C), C)
        act(load(wd_ref.at[layer, at, :], wdc.at[s], w_sem.at[s, 2]))

    def spills(j, act):
        s, at = j % 2, pl.ds(pl.multiple_of(j * C, C), C)
        act(load(hid.at[s], hid2_ref.at[at], out_sem.at[s, 0]))
        act(load(dg.at[s], dg2_ref.at[at], out_sem.at[s, 1]))
        act(load(du.at[s], du2_ref.at[at], out_sem.at[s, 2]))

    def row_loads(src, j, s, act):
        for d in range(8):
            rows = pl.ds(pl.multiple_of(d * (FF // 8) + j * RD, RD), RD)
            act(load(src.at[rows], hid.at[s, pl.ds(d * RD, RD)], row_sem.at[s, d]))

    def back_loads(j, s, act):
        at = pl.ds(pl.multiple_of(j * C, C), C)
        act(load(dg2_ref.at[at], dg.at[s], out_sem.at[s, 1]))
        act(load(du2_ref.at[at], du.at[s], out_sem.at[s, 2]))

    def gate1_loads(j, act):
        s, at = j % 2, pl.ds(pl.multiple_of(j * C, C), C)
        act(load(gate1_ref.at[at], acc.at[pl.ds(pl.multiple_of(s * 2 * C, C), C)], out_sem.at[s, 1]))
        act(load(up1_ref.at[at], acc.at[pl.ds(pl.multiple_of(s * 2 * C + C, C), C)], out_sem.at[s, 2]))

    def columns(i, size):
        return pl.ds(pl.multiple_of(i * size, size), size)

    def gate_gradient(t, a, d):
        s = t % SLOTS
        g = dot(a[...], d, ((1,), (1,))).astype(BF)
        for n in range(8):
            own[s, n % 2, n // 2] = g[n * RB : (n + 1) * RB]

    def down_gradient(t, rows, d):
        s = t % SLOTS

        @pl.loop(0, ND)
        def _(p):
            g = dot(rows, d[columns(p, C), :], ((1,), (1,))).astype(BF)
            for n in range(8):
                own[s, n % 2, n // 2, columns(p, RD), :] = g[n * RD : (n + 1) * RD]

    def produce(t):
        phase2 = t < EVEN1
        at = jnp.where(phase2, t, t - EVEN1)
        j = at // 2
        s = j % 2
        gate_even = (at < DOWN2) & (at % 2 == 0)
        gate_odd = (at < DOWN2) & (at % 2 == 1)

        @pl.when(phase2 & gate_even)
        def _():
            @pl.when(j == 0)
            def _():
                for i, (ref, to) in enumerate(((a2_ref, A), (dy_ref, B))):
                    load(ref, to, big_sem.at[i]).wait()
            gate_loads(1, j, wait)
            down_load(1, j, wait)

            @pl.when(j + 1 < NC)
            def _():
                gate_loads(1, j + 1, start)
                down_load(1, j + 1, start)

            @pl.when(j >= 2)
            def _():
                spills(j - 2, wait)

            @pl.loop(0, T // TT)
            def _(i):
                x = A[:, columns(i, TT)]
                gate = dot(wgc[s], x, ((0,), (0,)))
                up = dot(wuc[s], x, ((0,), (0,)))
                d_hidden = dot(wdc[s], B[:, columns(i, TT)], ((1,), (0,))).astype(BF).astype(F32)
                hid[s, :, columns(i, TT)], dg[s, :, columns(i, TT)], du[s, :, columns(i, TT)] = gates(gate, up, d_hidden)

            spills(j, start)
            gate_gradient(t, A, dg[s])

        @pl.when(phase2 & gate_odd)
        def _():
            gate_gradient(t, A, du[s])

            @pl.when(j == NC - 1)
            def _():
                spills(NC - 2, wait)
                spills(NC - 1, wait)
                gate_loads(1, 0, start)
                back_loads(0, NC % 2, start)
                row_loads(hid2_ref, 0, NC % 2, start)
                load(h1_ref, E, big_sem.at[2]).start()

        @pl.when(phase2 & (at >= DOWN2))
        def _():
            i = at - DOWN2
            n, other = (i + NC) % 2, (i + NC + 1) % 2
            gate_loads(1, i, wait)
            back_loads(i, n, wait)
            row_loads(hid2_ref, i, n, wait)

            @pl.when(i + 1 < NC)
            def _():
                gate_loads(1, i + 1, start)
                back_loads(i + 1, other, start)
                row_loads(hid2_ref, i + 1, other, start)

            down_gradient(t, hid[n], B)

            @pl.loop(0, T // TT)
            def _(x):
                cols = columns(x, TT)
                new = dot(wgc[i % 2], dg[n, :, cols], ((1,), (0,))) + dot(wuc[i % 2], du[n, :, cols], ((1,), (0,)))

                @pl.when(i == 0)
                def _():
                    acc[:, cols] = new

                @pl.when(i > 0)
                def _():
                    acc[:, cols] += new

            @pl.when(i == NC - 1)
            def _():
                load(h1_ref, E, big_sem.at[2]).wait()
                down_load(0, 0, start)
                TS = min(T, 128)

                @pl.loop(0, T // TS)
                def _(x):
                    cols = columns(x, TS)
                    h = E[:, cols].astype(F32)
                    da = acc[:, cols].astype(BF).astype(F32)
                    scale = lax.rsqrt(jnp.mean(h * h, 0, keepdims=True) + 1e-6)
                    inner = jnp.mean(da * h, 0, keepdims=True)
                    dh = (da * scale - h * (scale * scale * scale * inner)).astype(BF).astype(F32)
                    A[:, cols] = (B[:, cols].astype(F32) + dh).astype(BF)

                gate1_loads(0, start)
                load(a1_ref, E, big_sem.at[2]).start()

        @pl.when(~phase2 & gate_even)
        def _():
            down_load(0, j, wait)
            gate1_loads(j, wait)

            @pl.when(j + 1 < NC)
            def _():
                down_load(0, j + 1, start)
                gate1_loads(j + 1, start)

            @pl.loop(0, T // TT)
            def _(i):
                cols = columns(i, TT)
                gate, up = acc[columns(2 * s, C), cols], acc[columns(2 * s + 1, C), cols]
                d_hidden = dot(wdc[s], A[:, cols], ((1,), (0,))).astype(BF).astype(F32)
                _, dg[s, :, cols], du[s, :, cols] = gates(gate, up, d_hidden)

            @pl.when(j == 0)
            def _():
                load(a1_ref, E, big_sem.at[2]).wait()

            gate_gradient(t, E, dg[s])

        @pl.when(~phase2 & gate_odd)
        def _():
            @pl.when(j == NC - 1)
            def _():
                row_loads(hid1_ref, 0, 0, start)

            gate_gradient(t, E, du[s])

        @pl.when(~phase2 & (at >= DOWN2))
        def _():
            i = at - DOWN2
            row_loads(hid1_ref, i, i % 2, wait)

            @pl.when(i + 1 < NC)
            def _():
                row_loads(hid1_ref, i + 1, (i + 1) % 2, start)

            down_gradient(t, hid[i % 2], A)

    for i, (ref, to) in enumerate(((a2_ref, A), (dy_ref, B))):
        load(ref, to, big_sem.at[i]).start()
    gate_loads(1, 0, start)
    down_load(1, 0, start)

    @pl.when(c == 0)
    def _():
        R[:, 0] = jnp.zeros((SLOTS, RB, C), BF)

    @pl.when(c == CHIPS - 1)
    def _():
        L[:, CHIPS - 1] = jnp.zeros((SLOTS, RB, C), BF)

    pl.semaphore_wait(barrier, 1 + jnp.where(c > 0, 1, 0) + jnp.where(c < CHIPS - 1, 1, 0))

    @pl.loop(0, Q + 3 + 2 * HOP * (CHIPS - 1))
    def _(t):
        service(t)

        @pl.when(t < Q)
        def _():
            produce(t)
            ex_copy(t).start()


def mega(dims, *arrays):
    D, FF, T, C = dims
    Q, RB, RD, ND = 6 * (FF // C), D // 8, C // 8, D // C
    hbm = pl.BlockSpec(memory_space=pltpu.HBM)
    dma = lambda *shape: pltpu.SemaphoreType.DMA(shape)
    return pl.pallas_call(
        functools.partial(kernel, dims),
        out_shape=(
            jax.ShapeDtypeStruct((Q, 8, RB, C), BF),
            jax.ShapeDtypeStruct((Q, RB, C), F32),
            jax.ShapeDtypeStruct((Q, RB, C), F32),
        )
        + (jax.ShapeDtypeStruct((FF, T), BF),) * 3,
        in_specs=[hbm] * 16,
        out_specs=(hbm,) * 6,
        scratch_shapes=[pltpu.VMEM((D, T), BF)] * 3
        + [pltpu.VMEM((D, T), F32)]
        + [pltpu.VMEM((2, C, T), BF)] * 3
        + [pltpu.VMEM((2, D, C), BF)] * 2
        + [pltpu.VMEM((2, C, D), BF)]
        + [pltpu.VMEM((SLOTS, 2, CHIPS, RB, C), BF)]
        + [pltpu.VMEM((SLOTS, CHIPS, RB, C), BF)] * 3
        + [pltpu.VMEM((KEPT, RB, C), F32)] * 2
        + [pltpu.VMEM((KEPT, RB, C), BF)]
        + [pltpu.VMEM((KEPT, RB, C), F32)] * 2
        + [pltpu.VMEM((KEPT, RB, C), BF)]
        + [dma(SLOTS)] * 2
        + [dma(SLOTS, CHIPS)] * 10
        + [dma(3), dma(2, 3), dma(2, 8), dma(2, 3), dma(KEPT, 3, ND), dma(KEPT, 3)],
        compiler_params=pltpu.CompilerParams(collective_id=0, has_side_effects=True, vmem_limit_bytes=63 * 2**20),
        name="step",
    )(*arrays)[:3]


def place_kernel(dims, wg, wu, wd, mg, mu, md, vg, vu, vd, *outs):
    D, FF, T, C = dims
    RD, ND = C // 8, D // C
    for src, dst in ((wg, outs[0]), (wu, outs[1])):
        dst[...] = src[...].reshape(dst.shape)
    for src, dst in zip((mg, mu, vg, vu), (outs[3], outs[4], outs[6], outs[7])):
        dst[...] = src[...]
    for p in range(ND):
        rows, cols = slice(p * RD, (p + 1) * RD), slice(p * C, (p + 1) * C)
        outs[2][0, :, :, cols] = wd[0, :, rows]
        outs[5][0, :, cols] = md[0, rows]
        outs[8][0, :, cols] = vd[0, rows]


def place(dims, wp, mp, vp):
    D, FF, T, C = dims
    NC, RB, RD = FF // C, D // 8, C // 8
    first = lambda n: 3 * NC * (1 - n)
    chunk = (lambda n, j: first(n) + 2 * j, lambda n, j: first(n) + 2 * j + 1, lambda n, j: first(n) + 2 * NC + j)
    w_in = [pl.BlockSpec((1, 8, RB, C), lambda n, j, f=f: (f(n, j), 0, 0, 0)) for f in chunk]
    m_in = [pl.BlockSpec((1, RB, C), lambda n, j, f=f: (f(n, j), 0, 0)) for f in chunk]
    wide = lambda rows: pl.BlockSpec((1, rows, C), lambda n, j: (n, 0, j))
    w_out = [wide(D)] * 2 + [pl.BlockSpec((1, 8, RD, D), lambda n, j: (n, 0, j, 0))]
    m_out = [wide(RB)] * 2 + [pl.BlockSpec((1, RD, D), lambda n, j: (n, j, 0))]
    m_shapes = [jax.ShapeDtypeStruct((2, RB, FF), F32)] * 2 + [jax.ShapeDtypeStruct((2, FF // 8, D), F32)]
    outs = pl.pallas_call(
        functools.partial(place_kernel, dims),
        grid=(2, NC),
        in_specs=w_in + m_in + m_in,
        out_specs=w_out + m_out + m_out,
        out_shape=[jax.ShapeDtypeStruct((2, D, FF), BF)] * 2
        + [jax.ShapeDtypeStruct((2, 8, FF // 8, D), BF)]
        + m_shapes
        + m_shapes,
        compiler_params=pltpu.CompilerParams(vmem_limit_bytes=48 * 2**20),
        name="place",
    )(wp, wp, wp, mp, mp, mp, vp, vp, vp)
    outs = list(outs)
    outs[2] = outs[2].reshape(2, FF, D)
    return tuple(outs)


def solution(mesh):
    def local(x, dy, wg, wu, wd, mg, mu, md, vg, vu, vd):
        T, D = x.shape[1:]
        FF = wg.shape[2]
        dims = (D, FF, T, 256 if FF % 256 == 0 else 128)
        h0, dy = x[0].T, dy[0].T

        def normed(h):
            wide = h.astype(F32)
            return (wide * lax.rsqrt(jnp.mean(wide * wide, 0, keepdims=True) + 1e-6)).astype(BF)

        a1 = normed(h0)
        gate1 = dot(wg[0], a1, ((0,), (0,)))
        up1 = dot(wu[0], a1, ((0,), (0,)))
        hid1 = (jax.nn.silu(gate1) * up1).astype(BF)
        h1 = h0 + dot(wd[0], hid1, ((0,), (0,))).astype(BF)
        a2 = normed(h1)
        packed = mega(dims, a2, h1, dy, a1, hid1, gate1, up1, wg, wu, wd, mg, mu, md, vg, vu, vd)
        return place(dims, *packed)

    whole, rows, mine = P(None, None, None), P(None, "dp", None), P(("rep", "dp"), None, None)
    out_whole, out_rows = P("rep", None, None), P("rep", "dp", None)
    return jax.shard_map(
        local,
        mesh=mesh,
        in_specs=(mine, mine) + (whole,) * 3 + (rows,) * 6,
        out_specs=(out_whole,) * 3 + (out_rows,) * 6,
        check_vma=False,
    )
```

```python
import functools

import jax
import jax.numpy as jnp
from jax import lax
from jax.experimental import pallas as pl
from jax.experimental.pallas import tpu as pltpu
from jax.sharding import PartitionSpec as P

MESH = pl.DeviceIdType.MESH
BF, F32 = jnp.bfloat16, jnp.float32
CHIPS = 4
FIRST = 1
HOP = 1
SPREAD = 2
SLOTS = 11
ROWS = 2
RING = 16
KEPT = 3


def dot(a, b, dims):
    return lax.dot_general(a, b, (dims, ((), ())), preferred_element_type=F32)


def adamw(w, m, v, g):
    m = 0.9 * m + 0.1 * g
    v = 0.95 * v + 0.05 * g * g
    step = m * lax.rsqrt(v + 1e-8) + 0.1 * w
    return (w - 0.02 * step).astype(BF), m, v


def gates(gate, up, d_hidden):
    s = jax.nn.sigmoid(gate)
    gs = gate * s
    return (gs * up).astype(BF), (d_hidden * up * (s + gs * (1 - s))).astype(BF), (d_hidden * gs).astype(BF)


def kernel(dims, *refs):
    D, FF, T, C = dims
    x_ref, dy_ref, wg_ref, wu_ref, wd_ref = refs[:5]
    m_refs, v_refs = refs[5:8], refs[8:11]
    wp_ref, mp_ref, vp_ref, hid2_ref, dg2_ref, du2_ref = refs[11:17]
    (AT, BT, acc, rows, hid, dg, du, wgc, wuc, wdc, own, ex, R, L, mi, vi, wi, mo, vo, wo) = refs[17:37]
    (ex_s, ex_r, R_s, R_r, L_s, L_r, AR_s, AR_r, AL_s, AL_r, AD_s, AD_r) = refs[37:49]
    (w_sem, row_sem, out_sem, in_sem, put_sem, x_sem) = refs[49:]

    NC = FF // C
    Q = 6 * NC
    RB, RD, ND = D // 8, C // 8, D // C
    PAIRS = (NC + 1) // 2
    assert PAIRS + 4 <= NC
    DOWN, HALF = 2 * NC, 3 * NC
    TT = T // 2
    TR, TS = min(T, 256), min(TT, 256)
    later = pl.ds(TT, TT)
    parts = [slice(n * C, (n + 1) * C) for n in range(ND)]

    me = lax.axis_index("dp")
    c, k = me // 2, me % 2
    partner, right, left = me + 1 - 2 * k, me + 2, me - 2

    barrier = pltpu.get_barrier_semaphore()
    for there, ok in ((partner, None), (right, c < CHIPS - 1), (left, c > 0)):
        def greet(there=there):
            pl.semaphore_signal(barrier, inc=1, device_id={"dp": there}, device_id_type=MESH)
        greet() if ok is None else pl.when(ok)(greet)

    def load(src, dst, sem):
        return pltpu.make_async_copy(src, dst, sem)

    def send(src, dst, s, r, there):
        return pltpu.make_async_remote_copy(src, dst, s, r, device_id={"dp": there}, device_id_type=MESH)

    def chunk(t):
        return t, (t >= 0) & (t < Q)

    def end(b):
        return FIRST + HOP * jnp.maximum(b, CHIPS - 1 - b)

    def ex_copy(q):
        s = q % SLOTS
        return send(own.at[s, 1 - k], ex.at[s], ex_s.at[s], ex_r.at[s], partner)

    def R_copy(q, b):
        s = q % SLOTS
        return send(R.at[s, b], R.at[s, b], R_s.at[s, b], R_r.at[s, b], right)

    def L_copy(q, b):
        s = q % SLOTS
        return send(L.at[s, b], L.at[s, b], L_s.at[s, b], L_r.at[s, b], left)

    def all_gather_copy(q, b, there, s_sem, r_sem):
        s, at = q % SLOTS, wp_ref.at[q, 2 * b + k]
        return send(at, at, s_sem.at[s, b], r_sem.at[s, b], there)

    def AR_copy(q, b):
        return all_gather_copy(q, b, right, AR_s, AR_r)

    def AL_copy(q, b):
        return all_gather_copy(q, b, left, AL_s, AL_r)

    def AD_copy(q, b):
        return all_gather_copy(q, b, partner, AD_s, AD_r)

    def pieces(q, whole, wide):
        layer = jnp.where(q < HALF, 1, 0)
        at = jnp.where(q < HALF, q, q - HALF)
        for which in (0, 1):
            @pl.when((at < DOWN) & (at % 2 == which))
            def _():
                whole(which, layer, pl.multiple_of(at // 2 * C, C))
        @pl.when(at >= DOWN)
        def _():
            wide(2, layer, pl.multiple_of((at - DOWN) * RD, RD))

    def fetch(q, act):
        s = q % KEPT

        def whole(which, layer, column):
            cols = pl.ds(column, C)
            act(load(m_refs[which].at[layer, :, cols], mi.at[s], in_sem.at[s, 0, 0]))
            act(load(v_refs[which].at[layer, :, cols], vi.at[s], in_sem.at[s, 1, 0]))
            w = (wg_ref, wu_ref)[which]
            act(load(w.at[layer, pl.ds(pl.multiple_of(me * RB, RB), RB), cols], wi.at[s], in_sem.at[s, 2, 0]))

        def wide(which, layer, row):
            for p in range(ND):
                cols, to = pl.ds(p * C, C), pl.ds(p * RD, RD)
                act(load(m_refs[2].at[layer, pl.ds(row, RD), cols], mi.at[s, to], in_sem.at[s, 0, p]))
                act(load(v_refs[2].at[layer, pl.ds(row, RD), cols], vi.at[s, to], in_sem.at[s, 1, p]))
                rows = pl.ds(pl.multiple_of(me * (FF // 8) + row, RD), RD)
                act(load(wd_ref.at[layer, rows, cols], wi.at[s, to], in_sem.at[s, 2, p]))

        pieces(q, whole, wide)

    def puts(q):
        s = q % KEPT
        return (
            load(mo.at[s], mp_ref.at[q], put_sem.at[s, 0]),
            load(vo.at[s], vp_ref.at[q], put_sem.at[s, 1]),
            load(wo.at[s], wp_ref.at[q, me], put_sem.at[s, 2]),
        )

    def own_sends(q, act):
        s, n = q % KEPT, q % SLOTS
        to = wp_ref.at[q, me]

        @pl.when(c < CHIPS - 1)
        def _():
            act(send(wo.at[s], to, AR_s.at[n, c], AR_r.at[n, c], right))

        @pl.when(c > 0)
        def _():
            act(send(wo.at[s], to, AL_s.at[n, c], AL_r.at[n, c], left))

        act(send(wo.at[s], to, AD_s.at[n, c], AD_r.at[n, c], partner))

    def start(copy):
        copy.start()

    def wait(copy):
        copy.wait()

    def wait_send(copy):
        copy.wait_send()

    def service(t):
        new, is_new = chunk(t - FIRST)

        @pl.when(is_new)
        def _():
            ex_copy(new).wait_recv()

        q, is_q = chunk(t - FIRST - HOP * c)
        p, is_p = chunk(t - FIRST - HOP * (CHIPS - 1 - c))

        def up_sum(b):
            s = q % SLOTS
            terms = own[s, k, b].astype(F32) + ex[s, b].astype(F32)

            @pl.when(c == 0)
            def _():
                R[s, b] = terms.astype(BF)

            @pl.when(c > 0)
            def _():
                R_copy(q, b).wait_recv()
                R[s, b] = (terms + R[s, b].astype(F32)).astype(BF)

        def down_sum(b):
            s = p % SLOTS
            terms = own[s, k, b].astype(F32) + ex[s, b].astype(F32)

            @pl.when(c == CHIPS - 1)
            def _():
                L[s, b] = terms.astype(BF)

            @pl.when(c < CHIPS - 1)
            def _():
                L_copy(p, b).wait_recv()
                L[s, b] = (terms + L[s, b].astype(F32)).astype(BF)

        for n in range(CHIPS - 1):
            b = CHIPS - 1 - n
            go_up, go_down = is_q & (b > c), is_p & (n < c)

            @pl.when(go_up)
            def _():
                up_sum(b)

            @pl.when(go_down)
            def _():
                down_sum(n)

            @pl.when(go_up)
            def _():
                R_copy(q, b).start()

            @pl.when(go_down)
            def _():
                L_copy(p, n).start()

        q_e, gone_e = chunk(t - FIRST - HOP * (CHIPS - 1) - 2)

        @pl.when(gone_e)
        def _():
            ex_copy(q_e).wait_send()
            for b in range(CHIPS):
                if b > 0:
                    @pl.when(b > c)
                    def _():
                        R_copy(q_e, b).wait_send()
                if b < CHIPS - 1:
                    @pl.when(b < c)
                    def _():
                        L_copy(q_e, b).wait_send()

        q_o, gone_o = chunk(t - end(c) - 3)

        @pl.when(gone_o)
        def _():
            for copy in puts(q_o):
                copy.wait()
            own_sends(q_o, wait_send)

        q_m, ahead = chunk(t - end(c) + 2)

        @pl.when(ahead)
        def _():
            fetch(q_m, start)

        q_f, whole = chunk(t - end(c))

        @pl.when(whole)
        def _():
            @pl.when(c > 0)
            def _():
                R_copy(q_f, c).wait_recv()

            @pl.when(c < CHIPS - 1)
            def _():
                L_copy(q_f, c).wait_recv()

            fetch(q_f, wait)
            s, o = q_f % SLOTS, q_f % KEPT
            g = own[s, k, c].astype(F32) + ex[s, c].astype(F32) + R[s, c].astype(F32) + L[s, c].astype(F32)
            g = g.astype(BF).astype(F32)
            w, m, v = adamw(wi[o].astype(F32), mi[o], vi[o], g)
            wo[o], mo[o], vo[o] = w, m, v
            for copy in puts(q_f):
                copy.start()
            own_sends(q_f, start)

        for b in range(CHIPS):
            far = end(b) + SPREAD * jnp.abs(c - b)
            q_r, arrived = chunk(t - far)

            @pl.when((b < c) & arrived)
            def _():
                AR_copy(q_r, b).wait_recv()
                @pl.when(c < CHIPS - 1)
                def _():
                    AR_copy(q_r, b).start()
                AD_copy(q_r, b).start()

            @pl.when((b > c) & arrived)
            def _():
                AL_copy(q_r, b).wait_recv()
                @pl.when(c > 0)
                def _():
                    AL_copy(q_r, b).start()
                AD_copy(q_r, b).start()

            q_d, over = chunk(t - far - 1)

            @pl.when(over)
            def _():
                AD_copy(q_d, b).wait_recv()

            q_s, gone = chunk(t - far - 3)

            @pl.when(gone & (b != c))
            def _():
                @pl.when((b < c) & (c < CHIPS - 1))
                def _():
                    AR_copy(q_s, b).wait_send()
                @pl.when((b > c) & (c > 0))
                def _():
                    AL_copy(q_s, b).wait_send()
                AD_copy(q_s, b).wait_send()

    def chunk_of(j):
        return pl.ds(pl.multiple_of(j * C, C), C)

    def columns(i, size):
        return pl.ds(pl.multiple_of(i * size, size), size)

    def gate_loads(layer, j, n, act):
        act(load(wg_ref.at[layer, :, chunk_of(j)], wgc.at[n % 2], w_sem.at[n % 2, 0]))
        act(load(wu_ref.at[layer, :, chunk_of(j)], wuc.at[n % 2], w_sem.at[n % 2, 1]))

    def down_load(layer, j, n, act):
        act(load(wd_ref.at[layer, chunk_of(j), :], wdc.at[n % 2], w_sem.at[n % 2, 2]))

    def spills(j, act):
        s, at = j % 2, chunk_of(j)
        act(load(hid.at[s], hid2_ref.at[at], out_sem.at[s, 0]))
        act(load(dg.at[s, :, later], dg2_ref.at[at], out_sem.at[s, 1]))
        act(load(du.at[s, :, later], du2_ref.at[at], out_sem.at[s, 2]))

    def row_loads(i, act):
        for d in range(8):
            at = pl.ds(pl.multiple_of(d * (FF // 8) + i * RD, RD), RD)
            act(load(hid2_ref.at[at], hid.at[1 + i % 2, pl.ds(d * RD, RD)], row_sem.at[i % 2, d]))

    def back_loads(i, act):
        act(load(dg2_ref.at[chunk_of(i)], dg.at[i % 2, :, later], out_sem.at[i % 2, 1]))
        act(load(du2_ref.at[chunk_of(i)], du.at[i % 2, :, later], out_sem.at[i % 2, 2]))

    def token_load(ref, i, act):
        act(load(ref.at[columns(i, TR)], rows.at[i % ROWS], x_sem.at[i % ROWS]))

    def forward():
        NT = T // TR
        for i in range(min(ROWS, NT)):
            token_load(x_ref, i, start)
        gate_loads(0, 0, 0, start)
        down_load(0, 0, 0, start)

        @pl.loop(0, NT)
        def _(i):
            cols = columns(i, TR)
            token_load(x_ref, i, wait)
            total = jnp.zeros((1, TR), F32)
            for part in parts:
                h = rows[i % ROWS, :, part].T
                AT[1, part, cols] = h
                total += jnp.sum(h.astype(F32) ** 2, 0, keepdims=True)
            scale = lax.rsqrt(total / D + 1e-6)
            for part in parts:
                AT[0, part, cols] = (AT[1, part, cols].astype(F32) * scale).astype(BF)

            @pl.when(i + ROWS < NT)
            def _():
                token_load(x_ref, i + ROWS, start)

        for i in range(min(ROWS, NT)):
            token_load(dy_ref, i, start)

        @pl.loop(0, NC)
        def _(j):
            s = j % 2
            gate_loads(0, j, j, wait)
            down_load(0, j, j, wait)

            @pl.when(j + 1 < NC)
            def _():
                gate_loads(0, j + 1, j + 1, start)
                down_load(0, j + 1, j + 1, start)

            @pl.when(j + 1 == NC)
            def _():
                gate_loads(1, 0, NC, start)
                down_load(1, 0, NC, start)

            @pl.when(j < NT)
            def _():
                token_load(dy_ref, j, wait)

            tile = jnp.minimum(j, NT - 1)
            for part in parts:
                BT[1, part, columns(tile, TR)] = rows[tile % ROWS, :, part].T
            gate = dot(wgc[s], AT[0], ((0,), (0,)))
            up = dot(wuc[s], AT[0], ((0,), (0,)))
            hid[s] = (gate * jax.nn.sigmoid(gate) * up).astype(BF)

            @pl.loop(0, T // TT)
            def _(i):
                cols = columns(i, TT)
                acc[:, cols] = jnp.where(j > 0, acc[:, cols], 0.0) + dot(wdc[s], hid[s, :, cols], ((0,), (0,)))

            @pl.when(j + ROWS < NT)
            def _():
                token_load(dy_ref, j + ROWS, start)

        @pl.loop(0, T // TS)
        def _(i):
            cols = columns(i, TS)
            total = jnp.zeros((1, TS), F32)
            for part in parts:
                h = (AT[1, part, cols].astype(F32) + acc[part, cols].astype(BF).astype(F32)).astype(BF)
                BT[0, part, cols] = h
                total += jnp.sum(h.astype(F32) ** 2, 0, keepdims=True)
            scale = lax.rsqrt(total / D + 1e-6)
            for part in parts:
                AT[1, part, cols] = (BT[0, part, cols].astype(F32) * scale).astype(BF)

    def make_gates(layer, j, n, first, last):
        s = j % 2

        @pl.when(first == 0)
        def _():
            gate_loads(layer, j, n, wait)
            down_load(layer, j, n, wait)

            @pl.when(j + 1 < NC)
            def _():
                gate_loads(layer, j + 1, n + 1, start)
                down_load(layer, j + 1, n + 1, start)

            @pl.when(j >= 2)
            def _():
                spills(j - 2, wait)

        @pl.loop(first, last)
        def _(i):
            cols = columns(i, TT)
            gate = dot(wgc[n % 2], AT[layer, :, cols], ((0,), (0,)))
            up = dot(wuc[n % 2], AT[layer, :, cols], ((0,), (0,)))
            d_hidden = dot(wdc[n % 2], BT[layer, :, cols], ((1,), (0,))).astype(BF).astype(F32)
            hid[s, :, cols], dg[s, :, cols], du[s, :, cols] = gates(gate, up, d_hidden)

        @pl.when(last == 2)
        def _():
            spills(j, start)

    def into_normed(i, n, half):
        cols = columns(half, TT)
        from_gate = dot(wgc[n % 2], dg[i % 2, :, cols], ((1,), (0,)))
        from_up = dot(wuc[n % 2], du[i % 2, :, cols], ((1,), (0,)))
        acc[:, cols] = jnp.where(i > 0, acc[:, cols], 0.0) + (from_gate + from_up)

    def into_layer_1(half):
        @pl.loop(0, TT // TS)
        def _(i):
            cols = columns(half * (TT // TS) + i, TS)
            square, inner = jnp.zeros((1, TS), F32), jnp.zeros((1, TS), F32)
            for part in parts:
                h, da = BT[0, part, cols].astype(F32), acc[part, cols].astype(BF).astype(F32)
                square += jnp.sum(h * h, 0, keepdims=True)
                inner += jnp.sum(da * h, 0, keepdims=True)
            scale = lax.rsqrt(square / D + 1e-6)
            pull = scale * scale * scale * (inner / D)
            for part in parts:
                h, da = BT[0, part, cols].astype(F32), acc[part, cols].astype(BF).astype(F32)
                dh = (da * scale - h * pull).astype(BF).astype(F32)
                BT[0, part, cols] = (BT[1, part, cols].astype(F32) + dh).astype(BF)

    def produce(t):
        second = t < HALF
        layer = jnp.where(second, 1, 0)
        at = jnp.where(second, t, t - HALF)
        j, i = at // 2, at - DOWN

        @pl.when((at < DOWN) & (at % 2 == 0))
        def _():
            for n, d in ((0, dg), (1, du)):
                g = dot(AT[layer], d[j % 2], ((1,), (1,))).astype(BF)
                for e in range(8):
                    own[(t + n) % SLOTS, e % 2, e // 2] = g[e * RB : (e + 1) * RB]
            ex_copy(t).start()
            ex_copy(t + 1).start()

            @pl.when(second)
            def _():
                into_normed(j, NC + j, 0)

        @pl.when((at < DOWN) & (at % 2 == 1))
        def _():
            @pl.when(j + 1 < NC)
            def _():
                make_gates(layer, j + 1, jnp.where(second, NC, 3 * NC) + j + 1, 0, 2)

            @pl.when(j + 1 == NC)
            def _():
                if NC > 1:
                    spills(NC - 2, wait)
                spills(NC - 1, wait)
                row_loads(0, start)

                @pl.when(second)
                def _():
                    for n in range(2):
                        gate_loads(1, n, n, start)
                        back_loads(n, start)

        @pl.when(at >= DOWN)
        def _():
            row_loads(i, wait)

            @pl.when(i + 1 < NC)
            def _():
                row_loads(i + 1, start)

            g = dot(hid[1 + i % 2], BT[layer], ((1,), (1,))).astype(BF)
            for p in range(ND):
                for e in range(8):
                    own[t % SLOTS, e % 2, e // 2, p * RD : (p + 1) * RD] = g[e * RD : (e + 1) * RD, p * C : (p + 1) * C]
            ex_copy(t).start()

        @pl.when((at >= DOWN) & second & (i < PAIRS))
        def _():
            for n in range(2):
                @pl.when(2 * i + n < NC)
                def _():
                    gate_loads(1, 2 * i + n, n, wait)
                    back_loads(2 * i + n, wait)
                    into_normed(2 * i + n, n, 1)

                @pl.when(2 * i + n + 2 < NC)
                def _():
                    gate_loads(1, 2 * i + n + 2, n, start)
                    back_loads(2 * i + n + 2, start)

        @pl.when((at >= DOWN) & second & (i >= PAIRS) & (i < PAIRS + 2))
        def _():
            @pl.when(i == PAIRS)
            def _():
                gate_loads(0, 0, 3 * NC, start)
                down_load(0, 0, 3 * NC, start)

            into_layer_1(i - PAIRS)

        @pl.when((at >= DOWN) & second & (i >= PAIRS + 2) & (i < PAIRS + 4))
        def _():
            make_gates(0, 0, 3 * NC, i - PAIRS - 2, i - PAIRS - 1)

    @pl.when(c == 0)
    def _():
        R[:, 0] = jnp.zeros((SLOTS, RB, C), BF)

    @pl.when(c == CHIPS - 1)
    def _():
        L[:, CHIPS - 1] = jnp.zeros((SLOTS, RB, C), BF)

    forward()
    make_gates(1, 0, NC, 0, 2)
    pl.semaphore_wait(barrier, 1 + jnp.where(c > 0, 1, 0) + jnp.where(c < CHIPS - 1, 1, 0))

    @pl.loop(0, Q + FIRST + (HOP + SPREAD) * (CHIPS - 1) + 3)
    def _(t):
        service(t)

        @pl.when(t < Q)
        def _():
            produce(t)


def mega(dims, *arrays):
    D, FF, T, C = dims
    Q, RB, RD, ND = 6 * (FF // C), D // 8, C // 8, D // C
    hbm = pl.BlockSpec(memory_space=pltpu.HBM)
    dma = lambda *shape: pltpu.SemaphoreType.DMA(shape)
    return pl.pallas_call(
        functools.partial(kernel, dims),
        out_shape=(
            jax.ShapeDtypeStruct((Q, 8, RB, C), BF),
            jax.ShapeDtypeStruct((Q, RB, C), F32),
            jax.ShapeDtypeStruct((Q, RB, C), F32),
        )
        + (jax.ShapeDtypeStruct((FF, T), BF),)
        + (jax.ShapeDtypeStruct((FF, T // 2), BF),) * 2,
        in_specs=[hbm] * 11,
        out_specs=(hbm,) * 6,
        scratch_shapes=[pltpu.VMEM((2, D, T), BF)] * 2
        + [pltpu.VMEM((D, T), F32)]
        + [pltpu.VMEM((ROWS, min(T, 256), D), BF)]
        + [pltpu.VMEM((3, C, T), BF)]
        + [pltpu.VMEM((2, C, T), BF)] * 2
        + [pltpu.VMEM((2, D, C), BF)] * 2
        + [pltpu.VMEM((2, C, D), BF)]
        + [pltpu.VMEM((SLOTS, 2, CHIPS, RB, C), BF)]
        + [pltpu.VMEM((SLOTS, CHIPS, RB, C), BF)] * 3
        + [pltpu.VMEM((KEPT, RB, C), F32)] * 2
        + [pltpu.VMEM((KEPT, RB, C), BF)]
        + [pltpu.VMEM((KEPT, RB, C), F32)] * 2
        + [pltpu.VMEM((KEPT, RB, C), BF)]
        + [dma(SLOTS)] * 2
        + [dma(SLOTS, CHIPS)] * 10
        + [dma(2, 3), dma(2, 8), dma(2, 3), dma(KEPT, 3, ND), dma(KEPT, 3), dma(ROWS)],
        compiler_params=pltpu.CompilerParams(collective_id=0, has_side_effects=True, vmem_limit_bytes=67043328),
        name="step",
    )(*arrays)[:3]


def place_kernel(dims, *refs):
    D, FF, T, C = dims
    NC, RB, RD, ND = FF // C, D // 8, C // 8, D // C
    Q, HALF, DOWN = 6 * NC, 3 * NC, 2 * NC
    ins, outs, bufs, (in_sem, out_sem) = refs[:3], refs[3:12], refs[12:15], refs[15:]
    RING, LAG = bufs[0].shape[0], bufs[0].shape[0] // 2

    def copy_in(q, n):
        return pltpu.make_async_copy(ins[n].at[q], bufs[n].at[q % RING], in_sem.at[q % RING, n])

    def copies_out(q, act):
        layer = jnp.where(q < HALF, 1, 0)
        at = jnp.where(q < HALF, q, q - HALF)
        s = q % RING
        cols = pl.ds(pl.multiple_of(at // 2 * C, C), C)
        rows = pl.ds(pl.multiple_of((at - DOWN) * RD, RD), RD)
        for which in range(2):
            @pl.when((at < DOWN) & (at % 2 == which))
            def _():
                for n in range(3):
                    to = outs[3 * n + which]
                    to = to.at[layer, :, :, cols] if n == 0 else to.at[layer, :, cols]
                    act(pltpu.make_async_copy(bufs[n].at[s], to, out_sem.at[s, n, 0]))

        @pl.when(at >= DOWN)
        def _():
            for n in range(3):
                for p in range(ND):
                    piece, part = pl.ds(p * RD, RD), pl.ds(p * C, C)
                    if n == 0:
                        src, to = bufs[0].at[s, :, piece], outs[2].at[layer, :, rows, part]
                    else:
                        src, to = bufs[n].at[s, piece], outs[3 * n + 2].at[layer, rows, part]
                    act(pltpu.make_async_copy(src, to, out_sem.at[s, n, p]))

    @pl.loop(0, Q + RING)
    def _(q):
        @pl.when(q >= RING)
        def _():
            copies_out(q - RING, lambda copy: copy.wait())

        @pl.when(q < Q)
        def _():
            for n in range(3):
                copy_in(q, n).start()

        @pl.when((q >= LAG) & (q < Q + LAG))
        def _():
            for n in range(3):
                copy_in(q - LAG, n).wait()
            copies_out(q - LAG, lambda copy: copy.start())


def place(dims, wp, mp, vp):
    D, FF, T, C = dims
    RB, RD, ND = D // 8, C // 8, D // C
    hbm = pl.BlockSpec(memory_space=pltpu.HBM)
    states = [jax.ShapeDtypeStruct((2, RB, FF), F32)] * 2 + [jax.ShapeDtypeStruct((2, FF // 8, D), F32)]
    outs = pl.pallas_call(
        functools.partial(place_kernel, dims),
        in_specs=[hbm] * 3,
        out_specs=[hbm] * 9,
        out_shape=[jax.ShapeDtypeStruct((2, 8, RB, FF), BF)] * 2
        + [jax.ShapeDtypeStruct((2, 8, FF // 8, D), BF)]
        + states
        + states,
        scratch_shapes=[pltpu.VMEM((RING, 8, RB, C), BF)]
        + [pltpu.VMEM((RING, RB, C), F32)] * 2
        + [pltpu.SemaphoreType.DMA((RING, 3)), pltpu.SemaphoreType.DMA((RING, 3, ND))],
        compiler_params=pltpu.CompilerParams(vmem_limit_bytes=48 * 2**20),
        name="place",
    )(wp, mp, vp)
    return tuple(t.reshape(2, -1, t.shape[-1]) for t in outs)


def solution(mesh):
    def local(x, dy, wg, wu, wd, mg, mu, md, vg, vu, vd):
        T, D = x.shape[1:]
        FF = wg.shape[2]
        dims = (D, FF, T, 256 if FF % 256 == 0 else 128)
        return place(dims, *mega(dims, x[0], dy[0], wg, wu, wd, mg, mu, md, vg, vu, vd))

    whole, rows, mine = P(None, None, None), P(None, "dp", None), P(("rep", "dp"), None, None)
    out_whole, out_rows = P("rep", None, None), P("rep", "dp", None)
    return jax.shard_map(
        local,
        mesh=mesh,
        in_specs=(mine, mine) + (whole,) * 3 + (rows,) * 6,
        out_specs=(out_whole,) * 3 + (out_rows,) * 6,
        check_vma=False,
    )
```

```python
import functools

import jax
import jax.numpy as jnp
from jax import lax
from jax.experimental import pallas as pl
from jax.experimental.pallas import tpu as pltpu
from jax.sharding import PartitionSpec as P

MESH = pl.DeviceIdType.MESH
BF, F32 = jnp.bfloat16, jnp.float32
CHIPS = 4
FIRST = 1
HOP = 1
SPREAD = 2
SLOTS = 10
ROWS = 4
RING = 16
KEPT = 3


def dot(a, b, dims):
    return lax.dot_general(a, b, (dims, ((), ())), preferred_element_type=F32)


def adamw(w, m, v, g):
    m = 0.9 * m + 0.1 * g
    v = 0.95 * v + 0.05 * g * g
    step = m * lax.rsqrt(v + 1e-8) + 0.1 * w
    return (w - 0.02 * step).astype(BF), m, v


def gates(gate, up, d_hidden):
    s = jax.nn.sigmoid(gate)
    gs = gate * s
    return (gs * up).astype(BF), (d_hidden * up * (s + gs * (1 - s))).astype(BF), (d_hidden * gs).astype(BF)


def kernel(dims, *refs):
    D, FF, T, C = dims
    x_ref, dy_ref, wg_ref, wu_ref, wd_ref = refs[:5]
    m_refs, v_refs = refs[5:8], refs[8:11]
    wp_ref, mp_ref, vp_ref, hid2_ref, dg2_ref, du2_ref = refs[11:17]
    (AT, B, H, acc, rows, hid, dg, du, wgc, wuc, wdc, own, ex, R, L, mi, vi, wi, mo, vo, wo) = refs[17:38]
    (ex_s, ex_r, R_s, R_r, L_s, L_r, AR_s, AR_r, AL_s, AL_r, AD_s, AD_r) = refs[38:50]
    (w_sem, row_sem, out_sem, in_sem, put_sem, x_sem, dy_sem) = refs[50:]

    NC = FF // C
    Q = 6 * NC
    RB, RD, ND = D // 8, C // 8, D // C
    PAIRS = (NC + 1) // 2
    assert PAIRS + 3 <= NC
    DOWN, HALF = 2 * NC, 3 * NC
    TT = T // 2
    TR, TS = min(T // 4, 256), min(TT, 256)
    later = pl.ds(TT, TT)
    parts = [slice(n * C, (n + 1) * C) for n in range(ND)]

    me = lax.axis_index("dp")
    c, k = me // 2, me % 2
    partner, right, left = me + 1 - 2 * k, me + 2, me - 2

    barrier = pltpu.get_barrier_semaphore()
    for there, ok in ((partner, None), (right, c < CHIPS - 1), (left, c > 0)):
        def greet(there=there):
            pl.semaphore_signal(barrier, inc=1, device_id={"dp": there}, device_id_type=MESH)
        greet() if ok is None else pl.when(ok)(greet)

    def load(src, dst, sem):
        return pltpu.make_async_copy(src, dst, sem)

    def send(src, dst, s, r, there):
        return pltpu.make_async_remote_copy(src, dst, s, r, device_id={"dp": there}, device_id_type=MESH)

    def chunk(t):
        return t, (t >= 0) & (t < Q)

    def end(b):
        return FIRST + HOP * jnp.maximum(b, CHIPS - 1 - b)

    def ex_copy(q):
        s = q % SLOTS
        return send(own.at[s, 1 - k], ex.at[s], ex_s.at[s], ex_r.at[s], partner)

    def R_copy(q, b):
        s = q % SLOTS
        return send(R.at[s, b], R.at[s, b], R_s.at[s, b], R_r.at[s, b], right)

    def L_copy(q, b):
        s = q % SLOTS
        return send(L.at[s, b], L.at[s, b], L_s.at[s, b], L_r.at[s, b], left)

    def all_gather_copy(q, b, there, s_sem, r_sem):
        s, at = q % SLOTS, wp_ref.at[q, 2 * b + k]
        return send(at, at, s_sem.at[s, b], r_sem.at[s, b], there)

    def AR_copy(q, b):
        return all_gather_copy(q, b, right, AR_s, AR_r)

    def AL_copy(q, b):
        return all_gather_copy(q, b, left, AL_s, AL_r)

    def AD_copy(q, b):
        return all_gather_copy(q, b, partner, AD_s, AD_r)

    def pieces(q, whole, wide):
        layer = jnp.where(q < HALF, 1, 0)
        at = jnp.where(q < HALF, q, q - HALF)
        for which in (0, 1):
            @pl.when((at < DOWN) & (at % 2 == which))
            def _():
                whole(which, layer, pl.multiple_of(at // 2 * C, C))
        @pl.when(at >= DOWN)
        def _():
            wide(2, layer, pl.multiple_of((at - DOWN) * RD, RD))

    def fetch(q, act):
        s = q % KEPT

        def whole(which, layer, column):
            cols = pl.ds(column, C)
            act(load(m_refs[which].at[layer, :, cols], mi.at[s], in_sem.at[s, 0, 0]))
            act(load(v_refs[which].at[layer, :, cols], vi.at[s], in_sem.at[s, 1, 0]))
            w = (wg_ref, wu_ref)[which]
            act(load(w.at[layer, pl.ds(pl.multiple_of(me * RB, RB), RB), cols], wi.at[s], in_sem.at[s, 2, 0]))

        def wide(which, layer, row):
            for p in range(ND):
                cols, to = pl.ds(p * C, C), pl.ds(p * RD, RD)
                act(load(m_refs[2].at[layer, pl.ds(row, RD), cols], mi.at[s, to], in_sem.at[s, 0, p]))
                act(load(v_refs[2].at[layer, pl.ds(row, RD), cols], vi.at[s, to], in_sem.at[s, 1, p]))
                rows = pl.ds(pl.multiple_of(me * (FF // 8) + row, RD), RD)
                act(load(wd_ref.at[layer, rows, cols], wi.at[s, to], in_sem.at[s, 2, p]))

        pieces(q, whole, wide)

    def puts(q):
        s = q % KEPT
        return (
            load(mo.at[s], mp_ref.at[q], put_sem.at[s, 0]),
            load(vo.at[s], vp_ref.at[q], put_sem.at[s, 1]),
            load(wo.at[s], wp_ref.at[q, me], put_sem.at[s, 2]),
        )

    def own_sends(q, act):
        s, n = q % KEPT, q % SLOTS
        to = wp_ref.at[q, me]

        @pl.when(c < CHIPS - 1)
        def _():
            act(send(wo.at[s], to, AR_s.at[n, c], AR_r.at[n, c], right))

        @pl.when(c > 0)
        def _():
            act(send(wo.at[s], to, AL_s.at[n, c], AL_r.at[n, c], left))

        act(send(wo.at[s], to, AD_s.at[n, c], AD_r.at[n, c], partner))

    def start(copy):
        copy.start()

    def wait(copy):
        copy.wait()

    def wait_send(copy):
        copy.wait_send()

    def service(t):
        new, is_new = chunk(t - FIRST)

        @pl.when(is_new)
        def _():
            ex_copy(new).wait_recv()

        q, is_q = chunk(t - FIRST - HOP * c)
        p, is_p = chunk(t - FIRST - HOP * (CHIPS - 1 - c))

        def up_sum(b):
            s = q % SLOTS
            terms = own[s, k, b].astype(F32) + ex[s, b].astype(F32)

            @pl.when(c == 0)
            def _():
                R[s, b] = terms.astype(BF)

            @pl.when(c > 0)
            def _():
                R_copy(q, b).wait_recv()
                R[s, b] = (terms + R[s, b].astype(F32)).astype(BF)

        def down_sum(b):
            s = p % SLOTS
            terms = own[s, k, b].astype(F32) + ex[s, b].astype(F32)

            @pl.when(c == CHIPS - 1)
            def _():
                L[s, b] = terms.astype(BF)

            @pl.when(c < CHIPS - 1)
            def _():
                L_copy(p, b).wait_recv()
                L[s, b] = (terms + L[s, b].astype(F32)).astype(BF)

        for n in range(CHIPS - 1):
            b = CHIPS - 1 - n
            go_up, go_down = is_q & (b > c), is_p & (n < c)

            @pl.when(go_up)
            def _():
                up_sum(b)

            @pl.when(go_down)
            def _():
                down_sum(n)

            @pl.when(go_up)
            def _():
                R_copy(q, b).start()

            @pl.when(go_down)
            def _():
                L_copy(p, n).start()

        q_e, gone_e = chunk(t - FIRST - HOP * (CHIPS - 1) - 2)

        @pl.when(gone_e)
        def _():
            ex_copy(q_e).wait_send()
            for b in range(CHIPS):
                if b > 0:
                    @pl.when(b > c)
                    def _():
                        R_copy(q_e, b).wait_send()
                if b < CHIPS - 1:
                    @pl.when(b < c)
                    def _():
                        L_copy(q_e, b).wait_send()

        q_o, gone_o = chunk(t - end(c) - 3)

        @pl.when(gone_o)
        def _():
            for copy in puts(q_o):
                copy.wait()
            own_sends(q_o, wait_send)

        q_m, ahead = chunk(t - end(c) + 2)

        @pl.when(ahead)
        def _():
            fetch(q_m, start)

        q_f, whole = chunk(t - end(c))

        @pl.when(whole)
        def _():
            @pl.when(c > 0)
            def _():
                R_copy(q_f, c).wait_recv()

            @pl.when(c < CHIPS - 1)
            def _():
                L_copy(q_f, c).wait_recv()

            fetch(q_f, wait)
            s, o = q_f % SLOTS, q_f % KEPT
            g = own[s, k, c].astype(F32) + ex[s, c].astype(F32) + R[s, c].astype(F32) + L[s, c].astype(F32)
            g = g.astype(BF).astype(F32)
            w, m, v = adamw(wi[o].astype(F32), mi[o], vi[o], g)
            wo[o], mo[o], vo[o] = w, m, v
            for copy in puts(q_f):
                copy.start()
            own_sends(q_f, start)

        for b in range(CHIPS):
            far = end(b) + SPREAD * jnp.abs(c - b)
            q_r, arrived = chunk(t - far)

            @pl.when((b < c) & arrived)
            def _():
                AR_copy(q_r, b).wait_recv()
                @pl.when(c < CHIPS - 1)
                def _():
                    AR_copy(q_r, b).start()
                AD_copy(q_r, b).start()

            @pl.when((b > c) & arrived)
            def _():
                AL_copy(q_r, b).wait_recv()
                @pl.when(c > 0)
                def _():
                    AL_copy(q_r, b).start()
                AD_copy(q_r, b).start()

            q_d, over = chunk(t - far - 1)

            @pl.when(over)
            def _():
                AD_copy(q_d, b).wait_recv()

            q_s, gone = chunk(t - far - 3)

            @pl.when(gone & (b != c))
            def _():
                @pl.when((b < c) & (c < CHIPS - 1))
                def _():
                    AR_copy(q_s, b).wait_send()
                @pl.when((b > c) & (c > 0))
                def _():
                    AL_copy(q_s, b).wait_send()
                AD_copy(q_s, b).wait_send()

    def chunk_of(j):
        return pl.ds(pl.multiple_of(j * C, C), C)

    def columns(i, size):
        return pl.ds(pl.multiple_of(i * size, size), size)

    def gate_loads(layer, j, n, act):
        act(load(wg_ref.at[layer, :, chunk_of(j)], wgc.at[n % 2], w_sem.at[n % 2, 0]))
        act(load(wu_ref.at[layer, :, chunk_of(j)], wuc.at[n % 2], w_sem.at[n % 2, 1]))

    def down_load(layer, j, n, act):
        act(load(wd_ref.at[layer, chunk_of(j), :], wdc.at[n % 2], w_sem.at[n % 2, 2]))

    def spills(j, act):
        s, at = j % 2, chunk_of(j)
        act(load(hid.at[s], hid2_ref.at[at], out_sem.at[s, 0]))
        act(load(dg.at[s, :, later], dg2_ref.at[at], out_sem.at[s, 1]))
        act(load(du.at[s, :, later], du2_ref.at[at], out_sem.at[s, 2]))

    def row_loads(i, act):
        for d in range(8):
            at = pl.ds(pl.multiple_of(d * (FF // 8) + i * RD, RD), RD)
            act(load(hid2_ref.at[at], hid.at[1 + i % 2, pl.ds(d * RD, RD)], row_sem.at[i % 2, d]))

    def back_loads(i, act):
        act(load(dg2_ref.at[chunk_of(i)], dg.at[i % 2, :, later], out_sem.at[i % 2, 1]))
        act(load(du2_ref.at[chunk_of(i)], du.at[i % 2, :, later], out_sem.at[i % 2, 2]))

    def token_load(i, act):
        act(load(x_ref.at[columns(i, TR)], rows.at[i % ROWS], x_sem.at[i % ROWS]))

    def forward():
        quarters = range(4)
        TQ = T // 4

        def take_in(n):
            for i in range(n * (TQ // TR), (n + 1) * (TQ // TR)):
                cols = slice(i * TR, (i + 1) * TR)
                token_load(i, wait)
                total = jnp.zeros((1, TR), F32)
                for part in parts:
                    h = rows[i % ROWS, :, part].T
                    AT[1, part, cols] = h
                    total += jnp.sum(h.astype(F32) ** 2, 0, keepdims=True)
                scale = lax.rsqrt(total / D + 1e-6)
                for part in parts:
                    AT[0, part, cols] = (AT[1, part, cols].astype(F32) * scale).astype(BF)
                if i + ROWS < T // TR:
                    token_load(i + ROWS, start)

        def hidden(j, n):
            now = slice(n * TQ, (n + 1) * TQ)
            gate = dot(wgc[j % 2], AT[0, :, now], ((0,), (0,)))
            up = dot(wuc[j % 2], AT[0, :, now], ((0,), (0,)))
            hid[0, :, now] = (gate * jax.nn.sigmoid(gate) * up).astype(BF)

        def add(j, n):
            now = slice(n * TQ, (n + 1) * TQ)
            acc[:, now] = jnp.where(j > 0, acc[:, now], 0.0) + dot(wdc[j % 2], hid[0, :, now], ((0,), (0,)))

        def leave(n):
            for i in range(n * (TQ // TR), (n + 1) * (TQ // TR)):
                cols = slice(i * TR, (i + 1) * TR)
                total = jnp.zeros((1, TR), F32)
                for part in parts:
                    h = AT[1, part, cols] + acc[part, cols].astype(BF)
                    H[part, cols] = h
                    total += jnp.sum(h.astype(F32) ** 2, 0, keepdims=True)
                scale = lax.rsqrt(total / D + 1e-6)
                for part in parts:
                    AT[1, part, cols] = (H[part, cols].astype(F32) * scale).astype(BF)

        def staggered(steps):
            for n in range(4 + len(steps) - 1):
                for behind, step in enumerate(steps):
                    if n - behind in quarters:
                        step(n - behind)

        def weights(j, act):
            gate_loads(0, j, j, act)
            down_load(0, j, j, act)

        for i in range(min(ROWS, T // TR)):
            token_load(i, start)
        weights(0, start)
        load(dy_ref, B.at[1], dy_sem).start()
        weights(0, wait)
        weights(1, start)
        staggered((take_in, functools.partial(hidden, 0), functools.partial(add, 0)))

        @pl.loop(1, NC - 1)
        def _(j):
            weights(j, wait)
            weights(j + 1, start)
            staggered((functools.partial(hidden, j), functools.partial(add, j)))

        weights(NC - 1, wait)
        gate_loads(1, 0, NC, start)
        down_load(1, 0, NC, start)
        staggered((functools.partial(hidden, NC - 1), functools.partial(add, NC - 1), leave))

    def make_gates(layer, j, n):
        s = j % 2
        gate_loads(layer, j, n, wait)
        down_load(layer, j, n, wait)

        @pl.when(j + 1 < NC)
        def _():
            gate_loads(layer, j + 1, n + 1, start)
            down_load(layer, j + 1, n + 1, start)

        @pl.when(j >= 2)
        def _():
            spills(j - 2, wait)

        for i in range(2):
            cols = pl.ds(i * TT, TT)
            gate = dot(wgc[n % 2], AT[layer, :, cols], ((0,), (0,)))
            up = dot(wuc[n % 2], AT[layer, :, cols], ((0,), (0,)))
            d_hidden = dot(wdc[n % 2], B[layer, cols, :], ((1,), (1,))).astype(BF).astype(F32)
            hid[s, :, cols], dg[s, :, cols], du[s, :, cols] = gates(gate, up, d_hidden)

        spills(j, start)

    def into_normed(i, n, half):
        cols = columns(half, TT)
        from_gate = dot(wgc[n % 2], dg[i % 2, :, cols], ((1,), (0,)))
        from_up = dot(wuc[n % 2], du[i % 2, :, cols], ((1,), (0,)))
        acc[:, cols] = jnp.where(i > 0, acc[:, cols], 0.0) + (from_gate + from_up)

    def into_layer_1(half):
        @pl.loop(0, TT // TS)
        def _(i):
            cols = columns(half * (TT // TS) + i, TS)
            square, inner = jnp.zeros((1, TS), F32), jnp.zeros((1, TS), F32)
            for part in parts:
                h, da = H[part, cols].astype(F32), acc[part, cols].astype(BF).astype(F32)
                square += jnp.sum(h * h, 0, keepdims=True)
                inner += jnp.sum(da * h, 0, keepdims=True)
            scale = lax.rsqrt(square / D + 1e-6)
            pull = scale * scale * scale * (inner / D)
            for part in parts:
                h, da = H[part, cols].astype(F32), acc[part, cols].astype(BF).astype(F32)
                B[0, cols, part] = B[1, cols, part] + (da * scale - h * pull).astype(BF).T

    def produce(t):
        second = t < HALF
        layer = jnp.where(second, 1, 0)
        at = jnp.where(second, t, t - HALF)
        j, i = at // 2, at - DOWN

        @pl.when((at < DOWN) & (at % 2 == 0))
        def _():
            for n, d in ((0, dg), (1, du)):
                g = dot(AT[layer], d[j % 2], ((1,), (1,))).astype(BF)
                for e in range(8):
                    own[(t + n) % SLOTS, e % 2, e // 2] = g[e * RB : (e + 1) * RB]
            ex_copy(t).start()
            ex_copy(t + 1).start()

            @pl.when(second)
            def _():
                into_normed(j, NC + j, 0)

        @pl.when((at < DOWN) & (at % 2 == 1))
        def _():
            @pl.when(j + 1 == NC)
            def _():
                if NC > 1:
                    spills(NC - 2, wait)
                spills(NC - 1, wait)
                row_loads(0, start)

                @pl.when(second)
                def _():
                    for n in range(2):
                        gate_loads(1, n, n, start)
                        back_loads(n, start)

        @pl.when(at >= DOWN)
        def _():
            row_loads(i, wait)

            @pl.when(i + 1 < NC)
            def _():
                row_loads(i + 1, start)

            g = dot(hid[1 + i % 2], B[layer], ((1,), (0,))).astype(BF)
            for p in range(ND):
                for e in range(8):
                    own[t % SLOTS, e % 2, e // 2, p * RD : (p + 1) * RD] = g[e * RD : (e + 1) * RD, p * C : (p + 1) * C]
            ex_copy(t).start()

        @pl.when((at >= DOWN) & second & (i < PAIRS))
        def _():
            for n in range(2):
                @pl.when(2 * i + n < NC)
                def _():
                    gate_loads(1, 2 * i + n, n, wait)
                    back_loads(2 * i + n, wait)
                    into_normed(2 * i + n, n, 1)

                @pl.when(2 * i + n + 2 < NC)
                def _():
                    gate_loads(1, 2 * i + n + 2, n, start)
                    back_loads(2 * i + n + 2, start)

        @pl.when((at >= DOWN) & second & (i >= PAIRS) & (i < PAIRS + 2))
        def _():
            @pl.when(i == PAIRS)
            def _():
                gate_loads(0, 0, 3 * NC, start)
                down_load(0, 0, 3 * NC, start)

            into_layer_1(i - PAIRS)

        last = second & (i == PAIRS + 2)

        @pl.when(((at < DOWN) & (at % 2 == 1) & (j + 1 < NC)) | last)
        def _():
            n = jnp.where(second, NC, 3 * NC) + j + 1
            make_gates(jnp.where(last, 0, layer), jnp.where(last, 0, j + 1), jnp.where(last, 3 * NC, n))

    @pl.when(c == 0)
    def _():
        R[:, 0] = jnp.zeros((SLOTS, RB, C), BF)

    @pl.when(c == CHIPS - 1)
    def _():
        L[:, CHIPS - 1] = jnp.zeros((SLOTS, RB, C), BF)

    forward()
    load(dy_ref, B.at[1], dy_sem).wait()
    make_gates(1, 0, NC)
    pl.semaphore_wait(barrier, 1 + jnp.where(c > 0, 1, 0) + jnp.where(c < CHIPS - 1, 1, 0))

    @pl.loop(0, Q + FIRST + (HOP + SPREAD) * (CHIPS - 1) + 3)
    def _(t):
        service(t)

        @pl.when(t < Q)
        def _():
            produce(t)


def mega(dims, *arrays):
    D, FF, T, C = dims
    Q, RB, RD, ND = 6 * (FF // C), D // 8, C // 8, D // C
    hbm = pl.BlockSpec(memory_space=pltpu.HBM)
    dma = lambda *shape: pltpu.SemaphoreType.DMA(shape)
    return pl.pallas_call(
        functools.partial(kernel, dims),
        out_shape=(
            jax.ShapeDtypeStruct((Q, 8, RB, C), BF),
            jax.ShapeDtypeStruct((Q, RB, C), F32),
            jax.ShapeDtypeStruct((Q, RB, C), F32),
        )
        + (jax.ShapeDtypeStruct((FF, T), BF),)
        + (jax.ShapeDtypeStruct((FF, T // 2), BF),) * 2,
        in_specs=[hbm] * 11,
        out_specs=(hbm,) * 6,
        scratch_shapes=[pltpu.VMEM((2, D, T), BF), pltpu.VMEM((2, T, D), BF), pltpu.VMEM((D, T), BF)]
        + [pltpu.VMEM((D, T), F32)]
        + [pltpu.VMEM((ROWS, min(T // 4, 256), D), BF)]
        + [pltpu.VMEM((3, C, T), BF)]
        + [pltpu.VMEM((2, C, T), BF)] * 2
        + [pltpu.VMEM((2, D, C), BF)] * 2
        + [pltpu.VMEM((2, C, D), BF)]
        + [pltpu.VMEM((SLOTS, 2, CHIPS, RB, C), BF)]
        + [pltpu.VMEM((SLOTS, CHIPS, RB, C), BF)] * 3
        + [pltpu.VMEM((KEPT, RB, C), F32)] * 2
        + [pltpu.VMEM((KEPT, RB, C), BF)]
        + [pltpu.VMEM((KEPT, RB, C), F32)] * 2
        + [pltpu.VMEM((KEPT, RB, C), BF)]
        + [dma(SLOTS)] * 2
        + [dma(SLOTS, CHIPS)] * 10
        + [dma(2, 3), dma(2, 8), dma(2, 3), dma(KEPT, 3, ND), dma(KEPT, 3), dma(ROWS), pltpu.SemaphoreType.DMA],
        compiler_params=pltpu.CompilerParams(collective_id=0, has_side_effects=True, vmem_limit_bytes=67043328),
        name="step",
    )(*arrays)[:3]


def place_kernel(dims, *refs):
    D, FF, T, C = dims
    NC, RB, RD, ND = FF // C, D // 8, C // 8, D // C
    Q, HALF, DOWN = 6 * NC, 3 * NC, 2 * NC
    ins, outs, bufs, (in_sem, out_sem) = refs[:3], refs[3:12], refs[12:15], refs[15:]
    RING, LAG = bufs[0].shape[0], bufs[0].shape[0] // 2

    def copy_in(q, n):
        return pltpu.make_async_copy(ins[n].at[q], bufs[n].at[q % RING], in_sem.at[q % RING, n])

    def copies_out(q, act):
        layer = jnp.where(q < HALF, 1, 0)
        at = jnp.where(q < HALF, q, q - HALF)
        s = q % RING
        cols = pl.ds(pl.multiple_of(at // 2 * C, C), C)
        rows = pl.ds(pl.multiple_of((at - DOWN) * RD, RD), RD)
        for which in range(2):
            @pl.when((at < DOWN) & (at % 2 == which))
            def _():
                for n in range(3):
                    to = outs[3 * n + which]
                    to = to.at[layer, :, :, cols] if n == 0 else to.at[layer, :, cols]
                    act(pltpu.make_async_copy(bufs[n].at[s], to, out_sem.at[s, n, 0]))

        @pl.when(at >= DOWN)
        def _():
            for n in range(3):
                for p in range(ND):
                    piece, part = pl.ds(p * RD, RD), pl.ds(p * C, C)
                    if n == 0:
                        src, to = bufs[0].at[s, :, piece], outs[2].at[layer, :, rows, part]
                    else:
                        src, to = bufs[n].at[s, piece], outs[3 * n + 2].at[layer, rows, part]
                    act(pltpu.make_async_copy(src, to, out_sem.at[s, n, p]))

    @pl.loop(0, Q + RING)
    def _(q):
        @pl.when(q >= RING)
        def _():
            copies_out(q - RING, lambda copy: copy.wait())

        @pl.when(q < Q)
        def _():
            for n in range(3):
                copy_in(q, n).start()

        @pl.when((q >= LAG) & (q < Q + LAG))
        def _():
            for n in range(3):
                copy_in(q - LAG, n).wait()
            copies_out(q - LAG, lambda copy: copy.start())


def place(dims, wp, mp, vp):
    D, FF, T, C = dims
    RB, RD, ND = D // 8, C // 8, D // C
    hbm = pl.BlockSpec(memory_space=pltpu.HBM)
    states = [jax.ShapeDtypeStruct((2, RB, FF), F32)] * 2 + [jax.ShapeDtypeStruct((2, FF // 8, D), F32)]
    outs = pl.pallas_call(
        functools.partial(place_kernel, dims),
        in_specs=[hbm] * 3,
        out_specs=[hbm] * 9,
        out_shape=[jax.ShapeDtypeStruct((2, 8, RB, FF), BF)] * 2
        + [jax.ShapeDtypeStruct((2, 8, FF // 8, D), BF)]
        + states
        + states,
        scratch_shapes=[pltpu.VMEM((RING, 8, RB, C), BF)]
        + [pltpu.VMEM((RING, RB, C), F32)] * 2
        + [pltpu.SemaphoreType.DMA((RING, 3)), pltpu.SemaphoreType.DMA((RING, 3, ND))],
        compiler_params=pltpu.CompilerParams(vmem_limit_bytes=48 * 2**20),
        name="place",
    )(wp, mp, vp)
    return tuple(t.reshape(2, -1, t.shape[-1]) for t in outs)


def solution(mesh):
    def local(x, dy, wg, wu, wd, mg, mu, md, vg, vu, vd):
        T, D = x.shape[1:]
        FF = wg.shape[2]
        dims = (D, FF, T, 256 if FF % 256 == 0 else 128)
        return place(dims, *mega(dims, x[0], dy[0], wg, wu, wd, mg, mu, md, vg, vu, vd))

    whole, rows, mine = P(None, None, None), P(None, "dp", None), P(("rep", "dp"), None, None)
    out_whole, out_rows = P("rep", None, None), P("rep", "dp", None)
    return jax.shard_map(
        local,
        mesh=mesh,
        in_specs=(mine, mine) + (whole,) * 3 + (rows,) * 6,
        out_specs=(out_whole,) * 3 + (out_rows,) * 6,
        check_vma=False,
    )
```

```python
import functools

import jax
import jax.numpy as jnp
from jax import lax
from jax.experimental import pallas as pl
from jax.experimental.pallas import tpu as pltpu
from jax.sharding import PartitionSpec as P

MESH = pl.DeviceIdType.MESH
BF, F32 = jnp.bfloat16, jnp.float32
CHIPS = 4
FIRST = 1
HOP = 1
SPREAD = 2
SLOTS = 9
ROWS = 4
RING = 12
KEPT = 3


def dot(a, b, dims):
    return lax.dot_general(a, b, (dims, ((), ())), preferred_element_type=F32)


def adamw(w, m, v, g):
    m = 0.9 * m + 0.1 * g
    v = 0.95 * v + 0.05 * g * g
    step = m * lax.rsqrt(v + 1e-8) + 0.1 * w
    return (w - 0.02 * step).astype(BF), m, v


def gates(gate, up, d_hidden):
    s = jax.nn.sigmoid(gate)
    gs = gate * s
    return (gs * up).astype(BF), (d_hidden * up * (s + gs * (1 - s))).astype(BF), (d_hidden * gs).astype(BF)


def kernel(dims, *refs):
    D, FF, T, C = dims
    x_ref, dy_ref, wg_ref, wu_ref, wd_ref = refs[:5]
    m_refs, v_refs = refs[5:8], refs[8:11]
    wp_ref, mp_ref, vp_ref, hid2_ref, dg2_ref, du2_ref = refs[11:17]
    (AT, B, H, acc, rows, hid, dg, du, wgc, wuc, wdc, own, ex, R, L, mi, vi, wi, mo, vo, wo) = refs[17:38]
    (ex_s, ex_r, R_s, R_r, L_s, L_r, AR_s, AR_r, AL_s, AL_r, AD_s, AD_r) = refs[38:50]
    (w_sem, row_sem, out_sem, in_sem, put_sem, x_sem, dy_sem, turned, turned_down) = refs[50:]

    NC = FF // C
    Q = 6 * NC
    RB, RD, ND = D // 8, C // 8, D // C
    PAIRS = (NC + 1) // 2
    assert PAIRS + 4 <= NC
    DOWN, HALF = 2 * NC, 3 * NC
    TT = T // 2
    TR, TS = min(T // 4, 256), min(TT, 256)
    parts = [slice(n * C, (n + 1) * C) for n in range(ND)]

    me = lax.axis_index("dp")
    c, k = me // 2, me % 2
    partner, right, left = me + 1 - 2 * k, me + 2, me - 2

    barrier = pltpu.get_barrier_semaphore()
    for there, ok in ((partner, None), (right, c < CHIPS - 1), (left, c > 0)):
        def greet(there=there):
            pl.semaphore_signal(barrier, inc=1, device_id={"dp": there}, device_id_type=MESH)
        greet() if ok is None else pl.when(ok)(greet)

    def load(src, dst, sem):
        return pltpu.make_async_copy(src, dst, sem)

    def send(src, dst, s, r, there):
        return pltpu.make_async_remote_copy(src, dst, s, r, device_id={"dp": there}, device_id_type=MESH)

    def chunk(t):
        return t, (t >= 0) & (t < Q)

    def end(b):
        return FIRST + HOP * jnp.maximum(b, CHIPS - 1 - b)

    def ex_copy(q):
        s = q % SLOTS
        return send(own.at[s, 1 - k], ex.at[s], ex_s.at[s], ex_r.at[s], partner)

    def R_copy(q, b):
        s = q % SLOTS
        return send(R.at[s, b], R.at[s, b], R_s.at[s, b], R_r.at[s, b], right)

    def L_copy(q, b):
        s = q % SLOTS
        return send(L.at[s, b], L.at[s, b], L_s.at[s, b], L_r.at[s, b], left)

    def all_gather_copy(q, b, there, s_sem, r_sem):
        s, at = q % SLOTS, wp_ref.at[q, 2 * b + k]
        return send(at, at, s_sem.at[s, b], r_sem.at[s, b], there)

    def AR_copy(q, b):
        return all_gather_copy(q, b, right, AR_s, AR_r)

    def AL_copy(q, b):
        return all_gather_copy(q, b, left, AL_s, AL_r)

    def AD_copy(q, b):
        return all_gather_copy(q, b, partner, AD_s, AD_r)

    def pieces(q, whole, wide):
        layer = jnp.where(q < HALF, 1, 0)
        at = jnp.where(q < HALF, q, q - HALF)
        for which in (0, 1):
            @pl.when((at < DOWN) & (at % 2 == which))
            def _():
                whole(which, layer, pl.multiple_of(at // 2 * C, C))
        @pl.when(at >= DOWN)
        def _():
            wide(2, layer, pl.multiple_of((at - DOWN) * RD, RD))

    def fetch(q, act):
        s = q % KEPT

        def whole(which, layer, column):
            cols = pl.ds(column, C)
            act(load(m_refs[which].at[layer, :, cols], mi.at[s], in_sem.at[s, 0, 0]))
            act(load(v_refs[which].at[layer, :, cols], vi.at[s], in_sem.at[s, 1, 0]))
            w = (wg_ref, wu_ref)[which]
            act(load(w.at[layer, pl.ds(pl.multiple_of(me * RB, RB), RB), cols], wi.at[s], in_sem.at[s, 2, 0]))

        def wide(which, layer, row):
            for p in range(ND):
                cols, to = pl.ds(p * C, C), pl.ds(p * RD, RD)
                act(load(m_refs[2].at[layer, pl.ds(row, RD), cols], mi.at[s, to], in_sem.at[s, 0, p]))
                act(load(v_refs[2].at[layer, pl.ds(row, RD), cols], vi.at[s, to], in_sem.at[s, 1, p]))
                rows = pl.ds(pl.multiple_of(me * (FF // 8) + row, RD), RD)
                act(load(wd_ref.at[layer, rows, cols], wi.at[s, to], in_sem.at[s, 2, p]))

        pieces(q, whole, wide)

    def puts(q):
        s = q % KEPT
        return (
            load(mo.at[s], mp_ref.at[q], put_sem.at[s, 0]),
            load(vo.at[s], vp_ref.at[q], put_sem.at[s, 1]),
            load(wo.at[s], wp_ref.at[q, me], put_sem.at[s, 2]),
        )

    def own_sends(q, act):
        s, n = q % KEPT, q % SLOTS
        to = wp_ref.at[q, me]

        @pl.when(c < CHIPS - 1)
        def _():
            act(send(wo.at[s], to, AR_s.at[n, c], AR_r.at[n, c], right))

        @pl.when(c > 0)
        def _():
            act(send(wo.at[s], to, AL_s.at[n, c], AL_r.at[n, c], left))

        act(send(wo.at[s], to, AD_s.at[n, c], AD_r.at[n, c], partner))

    def start(copy):
        copy.start()

    def wait(copy):
        copy.wait()

    def wait_send(copy):
        copy.wait_send()

    def service(t):
        new, is_new = chunk(t - FIRST)

        @pl.when(is_new)
        def _():
            ex_copy(new).wait_recv()

        q, is_q = chunk(t - FIRST - HOP * c)
        p, is_p = chunk(t - FIRST - HOP * (CHIPS - 1 - c))

        def up_sum(b):
            s = q % SLOTS
            terms = own[s, k, b].astype(F32) + ex[s, b].astype(F32)

            @pl.when(c == 0)
            def _():
                R[s, b] = terms.astype(BF)

            @pl.when(c > 0)
            def _():
                R_copy(q, b).wait_recv()
                R[s, b] = (terms + R[s, b].astype(F32)).astype(BF)

        def down_sum(b):
            s = p % SLOTS
            terms = own[s, k, b].astype(F32) + ex[s, b].astype(F32)

            @pl.when(c == CHIPS - 1)
            def _():
                L[s, b] = terms.astype(BF)

            @pl.when(c < CHIPS - 1)
            def _():
                L_copy(p, b).wait_recv()
                L[s, b] = (terms + L[s, b].astype(F32)).astype(BF)

        def hop(n, act_up, act_down):
            b = CHIPS - 1 - n

            @pl.when(is_q & (b > c))
            def _():
                act_up(b)

            @pl.when(is_p & (n < c))
            def _():
                act_down(n)

        for n in range(CHIPS):
            if n < CHIPS - 1:
                hop(n, up_sum, down_sum)
            if n > 0:
                hop(n - 1, lambda b: R_copy(q, b).start(), lambda b: L_copy(p, b).start())

        q_e, gone_e = chunk(t - FIRST - HOP * (CHIPS - 1) - 2)

        @pl.when(gone_e)
        def _():
            ex_copy(q_e).wait_send()
            for b in range(CHIPS):
                if b > 0:
                    @pl.when(b > c)
                    def _():
                        R_copy(q_e, b).wait_send()
                if b < CHIPS - 1:
                    @pl.when(b < c)
                    def _():
                        L_copy(q_e, b).wait_send()

        q_o, gone_o = chunk(t - end(c) - 3)

        @pl.when(gone_o)
        def _():
            for copy in puts(q_o):
                copy.wait()
            own_sends(q_o, wait_send)

        q_m, ahead = chunk(t - end(c) + 2)

        @pl.when(ahead)
        def _():
            fetch(q_m, start)

        q_f, whole = chunk(t - end(c))

        @pl.when(whole)
        def _():
            @pl.when(c > 0)
            def _():
                R_copy(q_f, c).wait_recv()

            @pl.when(c < CHIPS - 1)
            def _():
                L_copy(q_f, c).wait_recv()

            fetch(q_f, wait)
            s, o = q_f % SLOTS, q_f % KEPT
            g = own[s, k, c].astype(F32) + ex[s, c].astype(F32) + R[s, c].astype(F32) + L[s, c].astype(F32)
            g = g.astype(BF).astype(F32)
            w, m, v = adamw(wi[o].astype(F32), mi[o], vi[o], g)
            wo[o], mo[o], vo[o] = w, m, v
            for copy in puts(q_f):
                copy.start()
            own_sends(q_f, start)

        for b in range(CHIPS):
            far = end(b) + SPREAD * jnp.abs(c - b)
            q_r, arrived = chunk(t - far)

            @pl.when((b < c) & arrived)
            def _():
                AR_copy(q_r, b).wait_recv()
                @pl.when(c < CHIPS - 1)
                def _():
                    AR_copy(q_r, b).start()
                AD_copy(q_r, b).start()

            @pl.when((b > c) & arrived)
            def _():
                AL_copy(q_r, b).wait_recv()
                @pl.when(c > 0)
                def _():
                    AL_copy(q_r, b).start()
                AD_copy(q_r, b).start()

            q_d, over = chunk(t - far - 1)

            @pl.when(over)
            def _():
                AD_copy(q_d, b).wait_recv()

            q_s, gone = chunk(t - far - 3)

            @pl.when(gone & (b != c))
            def _():
                @pl.when((b < c) & (c < CHIPS - 1))
                def _():
                    AR_copy(q_s, b).wait_send()
                @pl.when((b > c) & (c > 0))
                def _():
                    AL_copy(q_s, b).wait_send()
                AD_copy(q_s, b).wait_send()

    def chunk_of(j):
        return pl.ds(pl.multiple_of(j * C, C), C)

    def columns(i, size):
        return pl.ds(pl.multiple_of(i * size, size), size)

    def gate_loads(layer, j, n, act):
        act(load(wg_ref.at[layer, :, chunk_of(j)], wgc.at[n % 2], w_sem.at[n % 2, 0]))
        act(load(wu_ref.at[layer, :, chunk_of(j)], wuc.at[n % 2], w_sem.at[n % 2, 1]))

    def down_load(layer, j, n, act):
        act(load(wd_ref.at[layer, chunk_of(j), :], wdc.at[n % 2], w_sem.at[n % 2, 2]))

    def spills(j, act):
        s, at = j % 2, chunk_of(j)
        act(load(hid.at[s], hid2_ref.at[at], out_sem.at[s, 0]))
        act(load(dg.at[s], dg2_ref.at[at], out_sem.at[s, 1]))
        act(load(du.at[s], du2_ref.at[at], out_sem.at[s, 2]))

    def row_loads(i, act):
        for d in range(8):
            at = pl.ds(pl.multiple_of(d * (FF // 8) + i * RD, RD), RD)
            act(load(hid2_ref.at[at], hid.at[1 + i % 2, pl.ds(d * RD, RD)], row_sem.at[i % 2, d]))

    def back_loads(i, act):
        act(load(dg2_ref.at[chunk_of(i)], dg.at[i % 2], out_sem.at[i % 2, 1]))
        act(load(du2_ref.at[chunk_of(i)], du.at[i % 2], out_sem.at[i % 2, 2]))

    def token_load(i, act):
        act(load(x_ref.at[columns(i, TR)], rows.at[i % ROWS], x_sem.at[i % ROWS]))

    def forward():
        def tiles(n, size):
            return range(n * (size // TR), (n + 1) * (size // TR))

        def take_in(n, size):
            for i in tiles(n, size):
                cols = slice(i * TR, (i + 1) * TR)
                total = jnp.zeros((1, TR), F32)
                for part in parts:
                    h = rows[i % ROWS, :, part].T
                    AT[1, part, cols] = h
                    total += jnp.sum(h.astype(F32) ** 2, 0, keepdims=True)
                scale = lax.rsqrt(total / D + 1e-6)
                for part in parts:
                    AT[0, part, cols] = (AT[1, part, cols].astype(F32) * scale).astype(BF)

        FIRST_CHUNK = 0

        def turn():
            turned[0], turned[1] = wgc[0].T, wuc[0].T
            turned_down[...] = wdc[0].T

        def hidden(j, n, size):
            now = slice(n * size, (n + 1) * size)
            if j is FIRST_CHUNK:
                gate = dot(turned[0], AT[0, :, now], ((1,), (0,)))
                up = dot(turned[1], AT[0, :, now], ((1,), (0,)))
            else:
                gate = dot(wgc[j % 2], AT[0, :, now], ((0,), (0,)))
                up = dot(wuc[j % 2], AT[0, :, now], ((0,), (0,)))
            hid[0, :, now] = (gate * jax.nn.sigmoid(gate) * up).astype(BF)

        def add(j, n, size):
            now = slice(n * size, (n + 1) * size)
            if j is FIRST_CHUNK:
                acc[:, now] = dot(turned_down[...], hid[0, :, now], ((1,), (0,)))
            else:
                acc[:, now] = acc[:, now] + dot(wdc[j % 2], hid[0, :, now], ((0,), (0,)))

        def leave(n, size):
            for i in tiles(n, size):
                cols = slice(i * TR, (i + 1) * TR)
                total = jnp.zeros((1, TR), F32)
                for part in parts:
                    h = AT[1, part, cols] + acc[part, cols].astype(BF)
                    H[part, cols] = h
                    total += jnp.sum(h.astype(F32) ** 2, 0, keepdims=True)
                scale = lax.rsqrt(total / D + 1e-6)
                for part in parts:
                    AT[1, part, cols] = (H[part, cols].astype(F32) * scale).astype(BF)

        def weights(j, act):
            gate_loads(0, j, j, act)
            down_load(0, j, j, act)

        for i in range(min(ROWS, T // TR)):
            token_load(i, start)
        weights(0, start)
        FA, FZ = 4, 8
        FINE_A = T // FA
        for n in range(FA + 2):
            if n < FA:
                for i in tiles(n, FINE_A):
                    token_load(i, wait)
                take_in(n, FINE_A)
            if n == 1:
                weights(0, wait)
                turn()
            if 1 <= n < FA + 1:
                hidden(FIRST_CHUNK, n - 1, FINE_A)
            if n >= 2:
                add(FIRST_CHUNK, n - 2, FINE_A)
            if n < FA:
                for i in tiles(n, FINE_A):
                    if i + ROWS < T // TR:
                        token_load(i + ROWS, start)
            if n == 0:
                load(dy_ref, B.at[1], dy_sem).start()
                weights(1, start)

        @pl.loop(1, NC - 1)
        def _(j):
            weights(j, wait)
            weights(j + 1, start)
            for n in range(5):
                if n < 4:
                    hidden(j, n, T // 4)
                if n > 0:
                    add(j, n - 1, T // 4)

        weights(NC - 1, wait)
        gate_loads(1, 0, NC, start)
        down_load(1, 0, NC, start)
        FINE_Z = T // FZ
        for n in range(FZ + 2):
            if n < FZ:
                hidden(NC - 1, n, FINE_Z)
            if 1 <= n < FZ + 1:
                add(NC - 1, n - 1, FINE_Z)
            if n >= 2:
                leave(n - 2, FINE_Z)

    def make_gates(layer, j, n):
        s = j % 2
        gate_loads(layer, j, n, wait)
        down_load(layer, j, n, wait)

        @pl.when(j + 1 < NC)
        def _():
            gate_loads(layer, j + 1, n + 1, start)
            down_load(layer, j + 1, n + 1, start)

        @pl.when(j >= 2)
        def _():
            spills(j - 2, wait)

        for i in range(2):
            cols = pl.ds(i * TT, TT)
            gate = dot(wgc[n % 2], AT[layer, :, cols], ((0,), (0,)))
            up = dot(wuc[n % 2], AT[layer, :, cols], ((0,), (0,)))
            d_hidden = dot(wdc[n % 2], B[layer, cols, :], ((1,), (1,))).astype(BF).astype(F32)
            hid[s, :, cols], dg[s, :, cols], du[s, :, cols] = gates(gate, up, d_hidden)

        spills(j, start)

    def into_normed(i, n, half, fresh):
        cols = columns(half, TT)
        from_gate = dot(wgc[n % 2], dg[i % 2, :, cols], ((1,), (0,)))
        from_up = dot(wuc[n % 2], du[i % 2, :, cols], ((1,), (0,)))
        acc[:, cols] = jnp.where(fresh, 0.0, acc[:, cols]) + (from_gate + from_up)

    def into_layer_1(half):
        @pl.loop(0, TT // TS)
        def _(i):
            cols = columns(half * (TT // TS) + i, TS)
            square, inner = jnp.zeros((1, TS), F32), jnp.zeros((1, TS), F32)
            for part in parts:
                h, da = H[part, cols].astype(F32), acc[part, cols].astype(BF).astype(F32)
                square += jnp.sum(h * h, 0, keepdims=True)
                inner += jnp.sum(da * h, 0, keepdims=True)
            scale = lax.rsqrt(square / D + 1e-6)
            pull = scale * scale * scale * (inner / D)
            for part in parts:
                h, da = H[part, cols].astype(F32), acc[part, cols].astype(BF).astype(F32)
                B[0, cols, part] = B[1, cols, part] + (da * scale - h * pull).astype(BF).T

    def produce(t):
        second = t < HALF
        layer = jnp.where(second, 1, 0)
        at = jnp.where(second, t, t - HALF)
        j, i = at // 2, at - DOWN

        @pl.when((at < DOWN) & (at % 2 == 0))
        def _():
            for n, d in ((0, dg), (1, du)):
                g = dot(AT[layer], d[j % 2], ((1,), (1,))).astype(BF)
                for e in range(8):
                    own[(t + n) % SLOTS, e % 2, e // 2] = g[e * RB : (e + 1) * RB]
            ex_copy(t).start()
            ex_copy(t + 1).start()

            @pl.when(second & (j >= 2))
            def _():
                into_normed(j, NC + j, 0, j == 2)

        @pl.when((at < DOWN) & (at % 2 == 1))
        def _():
            @pl.when(j + 1 == NC)
            def _():
                if NC > 1:
                    spills(NC - 2, wait)
                spills(NC - 1, wait)
                row_loads(0, start)

                @pl.when(second)
                def _():
                    for n in range(2):
                        gate_loads(1, n, n, start)
                        back_loads(n, start)

        @pl.when(at >= DOWN)
        def _():
            row_loads(i, wait)

            @pl.when(i + 1 < NC)
            def _():
                row_loads(i + 1, start)

            g = dot(hid[1 + i % 2], B[layer], ((1,), (0,))).astype(BF)
            for p in range(ND):
                for e in range(8):
                    own[t % SLOTS, e % 2, e // 2, p * RD : (p + 1) * RD] = g[e * RD : (e + 1) * RD, p * C : (p + 1) * C]
            ex_copy(t).start()

        @pl.when((at >= DOWN) & second & (i == 0))
        def _():
            for n in range(2):
                gate_loads(1, n, n, wait)
                back_loads(n, wait)
                into_normed(n, n, 0, False)

        @pl.when((at >= DOWN) & second & (i >= 1) & (i <= PAIRS))
        def _():
            for n in range(2):
                x = 2 * (i - 1) + n

                @pl.when(x < NC)
                def _():
                    @pl.when(x >= 2)
                    def _():
                        gate_loads(1, x, n, wait)
                        back_loads(x, wait)

                    into_normed(x, n, 1, x == 0)

                @pl.when(x + 2 < NC)
                def _():
                    gate_loads(1, x + 2, n, start)
                    back_loads(x + 2, start)

        @pl.when((at >= DOWN) & second & (i > PAIRS) & (i <= PAIRS + 2))
        def _():
            @pl.when(i == PAIRS + 1)
            def _():
                gate_loads(0, 0, 3 * NC, start)
                down_load(0, 0, 3 * NC, start)

            into_layer_1(i - PAIRS - 1)

        last = second & (i == PAIRS + 3)

        @pl.when(((at < DOWN) & (at % 2 == 1) & (j + 1 < NC)) | last)
        def _():
            n = jnp.where(second, NC, 3 * NC) + j + 1
            make_gates(jnp.where(last, 0, layer), jnp.where(last, 0, j + 1), jnp.where(last, 3 * NC, n))

    @pl.when(c == 0)
    def _():
        R[:, 0] = jnp.zeros((SLOTS, RB, C), BF)

    @pl.when(c == CHIPS - 1)
    def _():
        L[:, CHIPS - 1] = jnp.zeros((SLOTS, RB, C), BF)

    forward()
    load(dy_ref, B.at[1], dy_sem).wait()
    make_gates(1, 0, NC)
    pl.semaphore_wait(barrier, 1 + jnp.where(c > 0, 1, 0) + jnp.where(c < CHIPS - 1, 1, 0))

    @pl.loop(0, Q + FIRST + (HOP + SPREAD) * (CHIPS - 1) + 3)
    def _(t):
        service(t)

        @pl.when(t < Q)
        def _():
            produce(t)


def mega(dims, *arrays):
    D, FF, T, C = dims
    Q, RB, RD, ND = 6 * (FF // C), D // 8, C // 8, D // C
    hbm = pl.BlockSpec(memory_space=pltpu.HBM)
    dma = lambda *shape: pltpu.SemaphoreType.DMA(shape)
    return pl.pallas_call(
        functools.partial(kernel, dims),
        out_shape=(
            jax.ShapeDtypeStruct((Q, 8, RB, C), BF),
            jax.ShapeDtypeStruct((Q, RB, C), F32),
            jax.ShapeDtypeStruct((Q, RB, C), F32),
        )
        + (jax.ShapeDtypeStruct((FF, T), BF),) * 3,
        in_specs=[hbm] * 11,
        out_specs=(hbm,) * 6,
        scratch_shapes=[pltpu.VMEM((2, D, T), BF), pltpu.VMEM((2, T, D), BF), pltpu.VMEM((D, T), BF)]
        + [pltpu.VMEM((D, T), F32)]
        + [pltpu.VMEM((ROWS, min(T // 4, 256), D), BF)]
        + [pltpu.VMEM((3, C, T), BF)]
        + [pltpu.VMEM((2, C, T), BF)] * 2
        + [pltpu.VMEM((2, D, C), BF)] * 2
        + [pltpu.VMEM((2, C, D), BF)]
        + [pltpu.VMEM((SLOTS, 2, CHIPS, RB, C), BF)]
        + [pltpu.VMEM((SLOTS, CHIPS, RB, C), BF)] * 3
        + [pltpu.VMEM((KEPT, RB, C), F32)] * 2
        + [pltpu.VMEM((KEPT, RB, C), BF)]
        + [pltpu.VMEM((KEPT, RB, C), F32)] * 2
        + [pltpu.VMEM((KEPT, RB, C), BF)]
        + [dma(SLOTS)] * 2
        + [dma(SLOTS, CHIPS)] * 10
        + [dma(2, 3), dma(2, 8), dma(2, 3), dma(KEPT, 3, ND), dma(KEPT, 3), dma(ROWS), pltpu.SemaphoreType.DMA]
        + [pltpu.VMEM((2, C, D), BF), pltpu.VMEM((D, C), BF)],
        compiler_params=pltpu.CompilerParams(collective_id=0, has_side_effects=True, vmem_limit_bytes=67043328),
        name="step",
    )(*arrays)[:3]


def place_kernel(dims, *refs):
    D, FF, T, C = dims
    NC, RB, RD, ND = FF // C, D // 8, C // 8, D // C
    Q, HALF, DOWN = 6 * NC, 3 * NC, 2 * NC
    ins, outs, bufs, (in_sem, out_sem) = refs[:3], refs[3:12], refs[12:15], refs[15:]
    RING, LAG = bufs[0].shape[0], bufs[0].shape[0] * 2 // 3

    def copy_in(q, n):
        return pltpu.make_async_copy(ins[n].at[q], bufs[n].at[q % RING], in_sem.at[q % RING, n])

    def copies_out(q, act):
        layer = jnp.where(q < HALF, 1, 0)
        at = jnp.where(q < HALF, q, q - HALF)
        s = q % RING
        cols = pl.ds(pl.multiple_of(at // 2 * C, C), C)
        rows = pl.ds(pl.multiple_of((at - DOWN) * RD, RD), RD)
        for which in range(2):
            @pl.when((at < DOWN) & (at % 2 == which))
            def _():
                for n in range(3):
                    to = outs[3 * n + which]
                    to = to.at[layer, :, :, cols] if n == 0 else to.at[layer, :, cols]
                    act(pltpu.make_async_copy(bufs[n].at[s], to, out_sem.at[s, n, 0]))

        @pl.when(at >= DOWN)
        def _():
            for n in range(3):
                for p in range(ND):
                    piece, part = pl.ds(p * RD, RD), pl.ds(p * C, C)
                    if n == 0:
                        src, to = bufs[0].at[s, :, piece], outs[2].at[layer, :, rows, part]
                    else:
                        src, to = bufs[n].at[s, piece], outs[3 * n + 2].at[layer, rows, part]
                    act(pltpu.make_async_copy(src, to, out_sem.at[s, n, p]))

    @pl.loop(0, Q + RING)
    def _(q):
        @pl.when(q >= RING)
        def _():
            copies_out(q - RING, lambda copy: copy.wait())

        @pl.when(q < Q)
        def _():
            for n in range(3):
                copy_in(q, n).start()

        @pl.when((q >= LAG) & (q < Q + LAG))
        def _():
            for n in range(3):
                copy_in(q - LAG, n).wait()
            copies_out(q - LAG, lambda copy: copy.start())


def place(dims, wp, mp, vp):
    D, FF, T, C = dims
    RB, RD, ND = D // 8, C // 8, D // C
    hbm = pl.BlockSpec(memory_space=pltpu.HBM)
    states = [jax.ShapeDtypeStruct((2, RB, FF), F32)] * 2 + [jax.ShapeDtypeStruct((2, FF // 8, D), F32)]
    outs = pl.pallas_call(
        functools.partial(place_kernel, dims),
        in_specs=[hbm] * 3,
        out_specs=[hbm] * 9,
        out_shape=[jax.ShapeDtypeStruct((2, 8, RB, FF), BF)] * 2
        + [jax.ShapeDtypeStruct((2, 8, FF // 8, D), BF)]
        + states
        + states,
        scratch_shapes=[pltpu.VMEM((RING, 8, RB, C), BF)]
        + [pltpu.VMEM((RING, RB, C), F32)] * 2
        + [pltpu.SemaphoreType.DMA((RING, 3)), pltpu.SemaphoreType.DMA((RING, 3, ND))],
        compiler_params=pltpu.CompilerParams(vmem_limit_bytes=48 * 2**20),
        name="place",
    )(wp, mp, vp)
    return tuple(t.reshape(2, -1, t.shape[-1]) for t in outs)


def solution(mesh):
    def local(x, dy, wg, wu, wd, mg, mu, md, vg, vu, vd):
        T, D = x.shape[1:]
        FF = wg.shape[2]
        dims = (D, FF, T, 256 if FF % 256 == 0 else 128)
        return place(dims, *mega(dims, x[0], dy[0], wg, wu, wd, mg, mu, md, vg, vu, vd))

    whole, rows, mine = P(None, None, None), P(None, "dp", None), P(("rep", "dp"), None, None)
    out_whole, out_rows = P("rep", None, None), P("rep", "dp", None)
    return jax.shard_map(
        local,
        mesh=mesh,
        in_specs=(mine, mine) + (whole,) * 3 + (rows,) * 6,
        out_specs=(out_whole,) * 3 + (out_rows,) * 6,
        check_vma=False,
    )
```
